16 devices in a mesh: rep: 2 (over y, z), dp: 8 (over x, core).
Axes of the slice: x: 4, y: 2, z: 1, core: 2. Of those that a mesh axis runs over, the one named last changes fastest.
The devices are a block of a 4x4x8 slice.
Arguments:
- x: bfloat16 [16, 2048, 512], P(('rep', 'dp')), parts along dimension 0
- dy: bfloat16 [16, 2048, 512], P(('rep', 'dp')), parts along dimension 0
- wq: bfloat16 [2, 512, 512], P(None, 'dp')
- wk: bfloat16 [2, 512, 512], P(None, 'dp')
- wv: bfloat16 [2, 512, 512], P(None, 'dp')
- wo: bfloat16 [2, 512, 512], P(None, 'dp')
- w_gate: bfloat16 [2, 512, 2048], P(None, 'dp')
- w_up: bfloat16 [2, 512, 2048], P(None, 'dp')
- w_down: bfloat16 [2, 2048, 512], P(None, 'dp')
- m_wq: float32 [2, 512, 512], P(None, 'dp')
- m_wk: float32 [2, 512, 512], P(None, 'dp')
- m_wv: float32 [2, 512, 512], P(None, 'dp')
- m_wo: float32 [2, 512, 512], P(None, 'dp')
- m_w_gate: float32 [2, 512, 2048], P(None, 'dp')
- m_w_up: float32 [2, 512, 2048], P(None, 'dp')
- m_w_down: float32 [2, 2048, 512], P(None, 'dp')
- v_wq: float32 [2, 512, 512], P(None, 'dp')
- v_wk: float32 [2, 512, 512], P(None, 'dp')
- v_wv: float32 [2, 512, 512], P(None, 'dp')
- v_wo: float32 [2, 512, 512], P(None, 'dp')
- v_w_gate: float32 [2, 512, 2048], P(None, 'dp')
- v_w_up: float32 [2, 512, 2048], P(None, 'dp')
- v_w_down: float32 [2, 2048, 512], P(None, 'dp')
Outputs:
- output 1: bfloat16 [4, 512, 512], P('rep', 'dp'), parts along dimension 0
- output 2: bfloat16 [4, 512, 512], P('rep', 'dp'), parts along dimension 0
- output 3: bfloat16 [4, 512, 512], P('rep', 'dp'), parts along dimension 0
- output 4: bfloat16 [4, 512, 512], P('rep', 'dp'), parts along dimension 0
- output 5: bfloat16 [4, 512, 2048], P('rep', 'dp'), parts along dimension 0
- output 6: bfloat16 [4, 512, 2048], P('rep', 'dp'), parts along dimension 0
- output 7: bfloat16 [4, 2048, 512], P('rep', 'dp'), parts along dimension 0
- output 8: float32 [4, 512, 512], P('rep', 'dp'), parts along dimension 0
- output 9: float32 [4, 512, 512], P('rep', 'dp'), parts along dimension 0
- output 10: float32 [4, 512, 512], P('rep', 'dp'), parts along dimension 0
- output 11: float32 [4, 512, 512], P('rep', 'dp'), parts along dimension 0
- output 12: float32 [4, 512, 2048], P('rep', 'dp'), parts along dimension 0
- output 13: float32 [4, 512, 2048], P('rep', 'dp'), parts along dimension 0
- output 14: float32 [4, 2048, 512], P('rep', 'dp'), parts along dimension 0
- output 15: float32 [4, 512, 512], P('rep', 'dp'), parts along dimension 0
- output 16: float32 [4, 512, 512], P('rep', 'dp'), parts along dimension 0
- output 17: float32 [4, 512, 512], P('rep', 'dp'), parts along dimension 0
- output 18: float32 [4, 512, 512], P('rep', 'dp'), parts along dimension 0
- output 19: float32 [4, 512, 2048], P('rep', 'dp'), parts along dimension 0
- output 20: float32 [4, 512, 2048], P('rep', 'dp'), parts along dimension 0
- output 21: float32 [4, 2048, 512], P('rep', 'dp'), parts along dimension 0
There are 2 independent parts. The reference program is written for one: setup_inputs(seed, part) draws one part's arguments, and reference() takes and returns one part's arrays. A program takes and returns all parts, laid end to end along the dimension named above; an argument that names none is the same for every part.
All inputs are finite; a program needn't handle non-finite values.
Results may differ from the reference program's by a relative error of at most 0.024.
Values are sent between devices in bfloat16 or wider.
A program may use at most 768 MiB of HBM per device.

```python
import jax
import jax.numpy as jnp
from jax import lax

SEQUENCES = 8
TOKENS = 2048
D = 512
HEADS = 4
KV_HEADS = 4
HEAD = 128
FF = 2048
LAYERS = 2
THETA = 10000
NAMES = ("wq", "wk", "wv", "wo", "w_gate", "w_up", "w_down")
SHAPES = {
    "wq": (LAYERS, D, HEADS * HEAD),
    "wk": (LAYERS, D, KV_HEADS * HEAD),
    "wv": (LAYERS, D, KV_HEADS * HEAD),
    "wo": (LAYERS, HEADS * HEAD, D),
    "w_gate": (LAYERS, D, FF),
    "w_up": (LAYERS, D, FF),
    "w_down": (LAYERS, FF, D),
}


def bump(key, n, height):
    away = (jnp.arange(n, dtype=jnp.int32) - jax.random.randint(key, (), 0, n, jnp.int32)) % n
    return jnp.where(away < n // 8, height, 1.0)


def together(key, own, strength):
    shared = jax.random.normal(key, own.shape[1:], jnp.float32)
    return (own + strength * shared) * lax.rsqrt(1 + strength * strength)


def setup_inputs(seed: int = 0, part: int = 0) -> dict:
    kx, kdy, ka, kb, kz, kf, kh, kl, *keys = jax.random.split(jax.random.key(seed), 8 + 3 * len(NAMES))
    kx, kdy, ka, kb = (jax.random.fold_in(k, part) for k in (kx, kdy, ka, kb))
    kw, km, kv = (keys[i::3] for i in range(3))
    shape = (SEQUENCES, TOKENS, D)
    much_x, much_dy = jax.random.uniform(kz, (2,), jnp.float32, 0.0, 1.0)
    loud = 2.0 ** jax.random.uniform(jax.random.fold_in(kz, 1), (), jnp.float32, -1.0, 2.0)
    layers = 2.0 ** jax.random.uniform(kl, (LAYERS, 1, 1), jnp.float32, -1.0, 1.0)
    times = {"wq": 1.0, "wk": 1.0, "wv": 2.0, "wo": layers, "w_gate": 1.0, "w_up": bump(kh, FF, 4.0), "w_down": layers}
    x = together(ka, jax.random.normal(kx, shape, jnp.float32), much_x) * bump(kf, D, 4.0)
    dy = together(kb, jax.random.normal(kdy, shape, jnp.float32), much_dy)
    drawn = {"x": x.astype(jnp.bfloat16), "dy": (loud * dy * (SEQUENCES * TOKENS) ** -0.5).astype(jnp.bfloat16)}
    for key, name in zip(kw, NAMES, strict=True):
        drawn[name] = (jax.random.normal(key, SHAPES[name], jnp.float32) * SHAPES[name][1] ** -0.5 * times[name]).astype(jnp.bfloat16)
    for key, name in zip(km, NAMES, strict=True):
        drawn[f"m_{name}"] = 0.1 * jax.random.normal(key, SHAPES[name], jnp.float32)
    for key, name in zip(kv, NAMES, strict=True):
        drawn[f"v_{name}"] = loud * loud * jax.random.uniform(key, SHAPES[name], jnp.float32, 0.2, 0.6)
    return drawn


def matmul(a, w):
    return jnp.dot(a, w, preferred_element_type=jnp.float32).astype(jnp.bfloat16)


def normed(h):
    wide = h.astype(jnp.float32)
    scale = lax.rsqrt(jnp.mean(wide**2, -1, keepdims=True) + 1e-6)
    return (wide * scale).astype(jnp.bfloat16)


def turned(t, theta):
    half = t.shape[-1] // 2
    angle = jnp.arange(t.shape[0], dtype=jnp.float32)[:, None] * theta ** (-jnp.arange(half, dtype=jnp.float32) / half)
    cos, sin = jnp.cos(angle)[:, None], jnp.sin(angle)[:, None]
    a, b = t[..., :half].astype(jnp.float32), t[..., half:].astype(jnp.float32)
    return jnp.concatenate([a * cos - b * sin, b * cos + a * sin], -1).astype(jnp.bfloat16)


def seen_by(q, k, v):
    tokens, kv = q.shape[0], k.shape[1]
    q = q.reshape(tokens, kv, -1, q.shape[-1])
    scores = jnp.einsum("tgsd,ugd->gstu", q.astype(jnp.float32), k.astype(jnp.float32)) * q.shape[-1] ** -0.5
    place = jnp.arange(tokens)
    weights = jax.nn.softmax(jnp.where(place[:, None] >= place, scores, -jnp.inf), -1).astype(jnp.bfloat16)
    return jnp.einsum("gstu,ugd->tgsd", weights.astype(jnp.float32), v.astype(jnp.float32)).astype(jnp.bfloat16).reshape(tokens, -1)


def layer(h, w):
    a = normed(h)
    q, k = (turned(matmul(a, w[name]).reshape(h.shape[0], -1, HEAD), THETA) for name in ("wq", "wk"))
    h = h + matmul(seen_by(q, k, matmul(a, w["wv"]).reshape(h.shape[0], -1, HEAD)), w["wo"])
    b = normed(h)
    gate = jnp.dot(b, w["w_gate"], preferred_element_type=jnp.float32)
    up = jnp.dot(b, w["w_up"], preferred_element_type=jnp.float32)
    return h + matmul((jax.nn.silu(gate) * up).astype(jnp.bfloat16), w["w_down"])


def adamw(w, m, v, g):
    m = 0.9 * m + 0.1 * g
    v = 0.95 * v + 0.05 * g * g
    step = m * lax.rsqrt(v + 1e-8) + 0.1 * w
    return (w - 0.02 * step).astype(jnp.bfloat16), m, v


def stack(weights, h):
    return lax.scan(lambda h, w: (layer(h, w), None), h, weights)[0]


def reference(x, dy, wq, wk, wv, wo, w_gate, w_up, w_down, m_wq, m_wk, m_wv, m_wo, m_w_gate, m_w_up, m_w_down, v_wq, v_wk, v_wv, v_wo, v_w_gate, v_w_up, v_w_down):
    weights = dict(zip(NAMES, (wq, wk, wv, wo, w_gate, w_up, w_down), strict=True))

    def take(so_far, sequence):
        h, by_y = sequence
        _, back = jax.vjp(stack, weights, h)
        by_weights, by_h = back(by_y)
        return jax.tree.map(lambda total, term: total + term.astype(jnp.float32), so_far, by_weights), by_h

    none_yet = {name: jnp.zeros(w.shape, jnp.float32) for name, w in weights.items()}
    by_weights, by_x = lax.scan(take, none_yet, (x, dy))
    gradients = [by_weights[name].astype(jnp.bfloat16).astype(jnp.float32) for name in NAMES]
    first = (m_wq, m_wk, m_wv, m_wo, m_w_gate, m_w_up, m_w_down)
    second = (v_wq, v_wk, v_wv, v_wo, v_w_gate, v_w_up, v_w_down)
    new = [adamw(weights[name].astype(jnp.float32), m, v, g) for name, m, v, g in zip(NAMES, first, second, gradients, strict=True)]
    return tuple(one[which] for which in range(3) for one in new)
```

```python
import functools

import jax
import jax.numpy as jnp
import numpy as np
from jax import lax
from jax.experimental import pallas as pl
from jax.experimental.pallas import tpu as pltpu
from jax.sharding import PartitionSpec as P

NEG = -1e30
HIDDEN = 2 * NEG
LOG2E = 1.4426950408889634
LN2 = 0.6931471805599453
VMEM = 60 * 2**20
HEAD = 128
THETA = 10000
EPS = 1e-6
F32, BF16 = jnp.float32, jnp.bfloat16


def _dot(a, b, ca, cb):
    return lax.dot_general(a, b, (((ca,), (cb,)), ((), ())), preferred_element_type=F32)


def _scale(wide):
    return lax.rsqrt(jnp.mean(wide * wide, -1, keepdims=True) + EPS)


def _norm_bwd(wide, scale, d_normed):
    dot = jnp.sum(d_normed * wide, -1, keepdims=True)
    return d_normed * scale - wide * (dot * scale * scale * scale * (1.0 / wide.shape[-1]))


def _table(tokens):
    half = HEAD // 2
    angle = np.arange(tokens, dtype=np.float64)[:, None] * float(THETA) ** (-np.arange(half, dtype=np.float64) / half)
    return np.concatenate([np.cos(angle), np.sin(angle)], 1).astype(np.float32)


def _turns(cs):
    first = lax.broadcasted_iota(jnp.int32, cs.shape, 1) < HEAD // 2
    other = pltpu.roll(cs, HEAD // 2, 1)
    return jnp.where(first, cs, other), jnp.where(first, -other, cs)


def _turn(t, c, s):
    heads = [t[:, i : i + HEAD] for i in range(0, t.shape[1], HEAD)]
    return jnp.concatenate([x * c + pltpu.roll(x, HEAD // 2, 1) * s for x in heads], 1)


def _whole(shape):
    return pl.BlockSpec(shape, lambda *_: (0,) * len(shape), pipeline_mode=pl.Buffered(1))


def _rows(size, width):
    return pl.BlockSpec((size, width), lambda t: (t, 0))


def _cost(flops, *arrays, exps=0):
    return pl.CostEstimate(flops=int(flops), transcendentals=int(exps), bytes_accessed=int(sum(a.size * a.dtype.itemsize for a in arrays)))


def _params(**more):
    return pltpu.CompilerParams(dimension_semantics=("arbitrary",), vmem_limit_bytes=VMEM, **more)


def _like(shape, dtype=BF16):
    return jax.ShapeDtypeStruct(shape, dtype)


def _qkv_kernel(h_ref, cs_ref, wq_ref, wk_ref, wv_ref, q_ref, k_ref, v_ref):
    wide = h_ref[...].astype(F32)
    a = (wide * _scale(wide)).astype(BF16)
    c, s = _turns(cs_ref[...])
    for w_ref, out in ((wq_ref, q_ref), (wk_ref, k_ref)):
        t = _dot(a, w_ref[...], 1, 0).astype(BF16).astype(F32)
        out[...] = _turn(t, c, s).astype(BF16)
    v_ref[...] = _dot(a, wv_ref[...], 1, 0).astype(BF16)


def qkv(h, cs, wq, wk, wv, tile=512):
    tokens, d = h.shape
    width = wq.shape[1]
    return pl.pallas_call(
        _qkv_kernel,
        grid=(tokens // tile,),
        in_specs=[_rows(tile, d), _rows(tile, HEAD)] + [_whole(wq.shape)] * 3,
        out_specs=[_rows(tile, width)] * 3,
        out_shape=[_like((tokens, width))] * 3,
        compiler_params=_params(),
        cost_estimate=_cost(6 * tokens * d * width, h, h, h, h, wq, wk, wv),
    )(h, cs, wq, wk, wv)


def _triangle(keys, queries):
    return lax.broadcasted_iota(jnp.int32, (keys, queries), 1) >= lax.broadcasted_iota(jnp.int32, (keys, queries), 0)


def _attend_kernel(q_ref, k_ref, v_ref, o_ref, lse_ref, top_s, mix_s, *, scale, block):
    iq = pl.program_id(0)
    heads = q_ref.shape[1] // HEAD
    e = scale * LOG2E
    lanes = [slice(i * HEAD, (i + 1) * HEAD) for i in range(heads)]
    top_s[...] = jnp.full(top_s.shape, NEG, F32)
    mix_s[...] = jnp.zeros_like(mix_s)

    def part(key, keys, query, queries, masked):
        here, cols = pl.ds(key, keys), slice(query, query + queries)
        scores = [_dot(k_ref[here, x], q_ref[cols, x], 1, 1) for x in lanes]
        ok = _triangle(keys, queries) if masked else None
        ones = jnp.ones((8, keys), BF16)
        weights, keeps = [], []
        for i, s in enumerate(scores):
            if masked:
                s = jnp.where(ok, s, HIDDEN)
            old = top_s[i : i + 1, cols]
            top = jnp.maximum(old, s.max(axis=0, keepdims=True))
            top_s[i : i + 1, cols] = top
            weights.append(jnp.exp2((s - top) * e).astype(BF16))
            keeps.append(jnp.exp2((old - top) * e))
        for i, (p, keep) in enumerate(zip(weights, keeps)):
            values = jnp.concatenate([v_ref[here, lanes[i]].T, ones], axis=0)
            mix_s[i, :, cols] = mix_s[i, :, cols] * keep + _dot(values, p, 1, 0)

    lax.fori_loop(0, iq, lambda j, _: part(pl.multiple_of(j * block, block), block, 0, block, False), None)
    half = block // 2
    base = pl.multiple_of(iq * block, block)
    part(base, half, 0, block, True)
    part(pl.multiple_of(base + half, half), half, half, half, True)
    for i, x in enumerate(lanes):
        total = mix_s[i, HEAD : HEAD + 1, :]
        o_ref[:, x] = (mix_s[i, :HEAD, :] * (1 / total)).T.astype(BF16)
        lse_ref[i : i + 1, :] = top_s[i : i + 1, :] * scale + jnp.log(total)


def attend(q, k, v, block=512):
    tokens, width = q.shape
    heads = width // HEAD
    return pl.pallas_call(
        functools.partial(_attend_kernel, scale=HEAD**-0.5, block=block),
        grid=(tokens // block,),
        in_specs=[_rows(block, width), _whole(k.shape), _whole(v.shape)],
        out_specs=[_rows(block, width), pl.BlockSpec((heads, block), lambda t: (0, t))],
        out_shape=[_like((tokens, width)), _like((heads, tokens), F32)],
        scratch_shapes=[pltpu.VMEM((heads, block), F32), pltpu.VMEM((heads, HEAD + 8, block), F32)],
        compiler_params=_params(),
        cost_estimate=_cost(4 * heads * tokens * tokens * HEAD, q, k, v, q, exps=heads * tokens * tokens),
    )(q, k, v)


def _ffn_kernel(o_ref, h_ref, wo_ref, wg_ref, wu_ref, wd_ref, h1_ref, h2_ref, g_ref, u_ref, *, chunk):
    h1 = (h_ref[...].astype(F32) + _dot(o_ref[...], wo_ref[...], 1, 0).astype(BF16).astype(F32)).astype(BF16)
    h1_ref[...] = h1
    wide = h1.astype(F32)
    b = (wide * _scale(wide)).astype(BF16)
    total = None
    for at in range(0, wg_ref.shape[1], chunk):
        here = slice(at, at + chunk)
        gate, up = _dot(b, wg_ref[:, here], 1, 0), _dot(b, wu_ref[:, here], 1, 0)
        g_ref[:, here] = gate
        u_ref[:, here] = up
        act = (gate * jax.nn.sigmoid(gate) * up).astype(BF16)
        term = _dot(act, wd_ref[here, :], 1, 0)
        total = term if total is None else total + term
    h2_ref[...] = (wide + total.astype(BF16).astype(F32)).astype(BF16)


def ffn(o, h, wo, wg, wu, wd, tile=256, chunk=512):
    tokens, d = h.shape
    width, hidden = o.shape[1], wg.shape[1]
    return pl.pallas_call(
        functools.partial(_ffn_kernel, chunk=chunk),
        grid=(tokens // tile,),
        in_specs=[_rows(tile, width), _rows(tile, d)] + [_whole(w.shape) for w in (wo, wg, wu, wd)],
        out_specs=[_rows(tile, d)] * 2 + [_rows(tile, hidden)] * 2,
        out_shape=[_like((tokens, d))] * 2 + [_like((tokens, hidden), F32)] * 2,
        compiler_params=_params(),
        cost_estimate=_cost(2 * tokens * d * (width + 3 * hidden), o, h, h, h, wo, wg, wu, wd),
    )(o, h, wo, wg, wu, wd)


def _ffn_bwd_kernel(dh2_ref, h1_ref, g_ref, u_ref, o_ref, wo_ref, wg_ref, wu_ref, wd_ref,
                    dh1_ref, do_ref, dwo_ref, dwg_ref, dwu_ref, dwd_ref, awo, awg, awu, awd, *, chunk):
    t = pl.program_id(0)

    @pl.when(t == 0)
    def _():
        for acc in (awo, awg, awu, awd):
            acc[...] = jnp.zeros_like(acc)

    dh2 = dh2_ref[...]
    wide = h1_ref[...].astype(F32)
    scale = _scale(wide)
    b = (wide * scale).astype(BF16)
    db = None
    for at in range(0, wg_ref.shape[1], chunk):
        here = slice(at, at + chunk)
        d_act = _dot(dh2, wd_ref[here, :], 1, 1).astype(BF16).astype(F32)
        gate, up = g_ref[:, here], u_ref[:, here]
        sig = jax.nn.sigmoid(gate)
        silu = gate * sig
        act = (silu * up).astype(BF16)
        d_up = (d_act * silu).astype(BF16)
        d_gate = (d_act * up * (sig + silu * (1 - sig))).astype(BF16)
        term = _dot(d_gate, wg_ref[:, here], 1, 1) + _dot(d_up, wu_ref[:, here], 1, 1)
        db = term if db is None else db + term
        awd[here, :] += _dot(act, dh2, 0, 0)
        awg[:, here] += _dot(b, d_gate, 0, 0)
        awu[:, here] += _dot(b, d_up, 0, 0)
    db = db.astype(BF16).astype(F32)
    dh1 = (dh2.astype(F32) + _norm_bwd(wide, scale, db).astype(BF16).astype(F32)).astype(BF16)
    dh1_ref[...] = dh1
    do_ref[...] = _dot(dh1, wo_ref[...], 1, 1).astype(BF16)
    awo[...] += _dot(o_ref[...], dh1, 0, 0)

    @pl.when(t == pl.num_programs(0) - 1)
    def _():
        for out, acc in ((dwo_ref, awo), (dwg_ref, awg), (dwu_ref, awu), (dwd_ref, awd)):
            out[...] = acc[...].astype(BF16)


def ffn_bwd(dh2, h1, g, u, o, wo, wg, wu, wd, tile=256, chunk=512):
    tokens, d = h1.shape
    width, hidden = o.shape[1], wg.shape[1]
    ws = (wo, wg, wu, wd)
    return pl.pallas_call(
        functools.partial(_ffn_bwd_kernel, chunk=chunk),
        grid=(tokens // tile,),
        in_specs=[_rows(tile, d), _rows(tile, d), _rows(tile, hidden), _rows(tile, hidden), _rows(tile, width)] + [_whole(w.shape) for w in ws],
        out_specs=[_rows(tile, d), _rows(tile, width)] + [_whole(w.shape) for w in ws],
        out_shape=[_like((tokens, d)), _like((tokens, width))] + [_like(w.shape) for w in ws],
        scratch_shapes=[pltpu.VMEM(w.shape, F32) for w in ws],
        compiler_params=_params(),
        cost_estimate=_cost(4 * tokens * d * (width + 3 * hidden), g, u, h1, h1, h1, *ws, *ws),
    )(dh2, h1, g, u, o, *ws)


def _attend_bwd_kernel(q_ref, k_ref, v_ref, do_ref, o_ref, lse_ref, dq_ref, dk_ref, dv_ref, dq_s, dk_s, dv_s, *, scale, block):
    iq = pl.program_id(0)
    heads = q_ref.shape[1] // HEAD
    e = scale * LOG2E
    lanes = [slice(i * HEAD, (i + 1) * HEAD) for i in range(heads)]

    @pl.when(iq == 0)
    def _():
        dk_s[...] = jnp.zeros_like(dk_s)
        dv_s[...] = jnp.zeros_like(dv_s)

    dq_s[...] = jnp.zeros_like(dq_s)
    lses = [lse_ref[i : i + 1, :] * LOG2E for i in range(heads)]
    deltas = [(do_ref[:, x].astype(F32) * o_ref[:, x].astype(F32)).T.sum(axis=0, keepdims=True) for x in lanes]

    def part(key, keys, query, queries, masked):
        here, cols = pl.ds(key, keys), slice(query, query + queries)
        scores = [_dot(k_ref[here, x], q_ref[cols, x], 1, 1) for x in lanes]
        dps = [_dot(v_ref[here, x], do_ref[cols, x], 1, 1) for x in lanes]
        ok = _triangle(keys, queries) if masked else None
        for i, x in enumerate(lanes):
            p = jnp.exp2(scores[i] * e - lses[i][:, cols])
            if masked:
                p = jnp.where(ok, p, 0.0)
            ds = (p * (dps[i] - deltas[i][:, cols])).astype(BF16)
            dv_s[here, x] += _dot(p.astype(BF16), do_ref[cols, x], 1, 0)
            dk_s[here, x] += _dot(ds, q_ref[cols, x], 1, 0)
            dq_s[i, :, cols] += _dot(k_ref[here, x].T, ds, 1, 0)

    lax.fori_loop(0, iq, lambda j, _: part(pl.multiple_of(j * block, block), block, 0, block, False), None)
    half = block // 2
    base = pl.multiple_of(iq * block, block)
    part(base, half, 0, block, True)
    part(pl.multiple_of(base + half, half), half, half, half, True)
    for i, x in enumerate(lanes):
        dq_ref[:, x] = (dq_s[i] * scale).T.astype(BF16)

    @pl.when(iq == pl.num_programs(0) - 1)
    def _():
        dk_ref[...] = (dk_s[...] * scale).astype(BF16)
        dv_ref[...] = dv_s[...].astype(BF16)


def attend_bwd(q, k, v, do, o, lse, block=512):
    tokens, width = q.shape
    heads = width // HEAD
    return pl.pallas_call(
        functools.partial(_attend_bwd_kernel, scale=HEAD**-0.5, block=block),
        grid=(tokens // block,),
        in_specs=[_rows(block, width), _whole(k.shape), _whole(v.shape), _rows(block, width), _rows(block, width),
                  pl.BlockSpec((heads, block), lambda t: (0, t))],
        out_specs=[_rows(block, width), _whole(k.shape), _whole(v.shape)],
        out_shape=[_like((tokens, width))] * 3,
        scratch_shapes=[pltpu.VMEM((heads, HEAD, block), F32), pltpu.VMEM(k.shape, F32), pltpu.VMEM(v.shape, F32)],
        compiler_params=_params(),
        cost_estimate=_cost(10 * heads * tokens * tokens * HEAD, q, k, v, do, o, q, k, v, exps=heads * tokens * tokens),
    )(q, k, v, do, o, lse)


def _qkv_bwd_kernel(h_ref, cs_ref, dq_ref, dk_ref, dv_ref, *rest, inner):
    if inner:
        dh1_ref, wq_ref, wk_ref, wv_ref, dh_ref, dwq_ref, dwk_ref, dwv_ref, *accs = rest
    else:
        dwq_ref, dwk_ref, dwv_ref, *accs = rest
    t = pl.program_id(0)

    @pl.when(t == 0)
    def _():
        for acc in accs:
            acc[...] = jnp.zeros_like(acc)

    wide = h_ref[...].astype(F32)
    scale = _scale(wide)
    a = (wide * scale).astype(BF16)
    c, s = _turns(cs_ref[...])
    grads = [_turn(ref[...].astype(F32), c, -s).astype(BF16) for ref in (dq_ref, dk_ref)] + [dv_ref[...]]
    for acc, g in zip(accs, grads):
        acc[...] += _dot(a, g, 0, 0)
    if inner:
        da = sum(_dot(g, w[...], 1, 1) for g, w in zip(grads, (wq_ref, wk_ref, wv_ref)))
        da = da.astype(BF16).astype(F32)
        dh_ref[...] = (dh1_ref[...].astype(F32) + _norm_bwd(wide, scale, da).astype(BF16).astype(F32)).astype(BF16)

    @pl.when(t == pl.num_programs(0) - 1)
    def _():
        for out, acc in zip((dwq_ref, dwk_ref, dwv_ref), accs):
            out[...] = acc[...].astype(BF16)


def qkv_bwd(h, cs, dq, dk, dv, dh1=None, ws=None, tile=512):
    tokens, d = h.shape
    width = dq.shape[1]
    inner = dh1 is not None
    given = [h, cs, dq, dk, dv] + ([dh1, *ws] if inner else [])
    specs = [_rows(tile, d), _rows(tile, HEAD)] + [_rows(tile, width)] * 3 + ([_rows(tile, d)] + [_whole((d, width))] * 3 if inner else [])
    return pl.pallas_call(
        functools.partial(_qkv_bwd_kernel, inner=inner),
        grid=(tokens // tile,),
        in_specs=specs,
        out_specs=([_rows(tile, d)] if inner else []) + [_whole((d, width))] * 3,
        out_shape=([_like((tokens, d))] if inner else []) + [_like((d, width))] * 3,
        scratch_shapes=[pltpu.VMEM((d, width), F32)] * 3,
        compiler_params=_params(),
        cost_estimate=_cost((12 if inner else 6) * tokens * d * width, *given),
    )(*given)


def adamw(w, m, v, g):
    m = 0.9 * m + 0.1 * g
    v = 0.95 * v + 0.05 * g * g
    step = m * lax.rsqrt(v + 1e-8) + 0.1 * w
    return (w - 0.02 * step).astype(BF16), m, v


def solution(mesh):
    def gather(*blocks):
        got = lax.all_gather(jnp.stack(blocks), "dp", axis=1, tiled=True)
        return [got[i] for i in range(len(blocks))]

    def scatter(*grads):
        got = lax.psum_scatter(jnp.stack(grads), "dp", scatter_dimension=1, tiled=True)
        return [got[i] for i in range(len(grads))]

    def step(x, dy, *arrays):
        weights, m, v = (arrays[i : i + 7] for i in (0, 7, 14))
        layers = weights[0].shape[0]
        h = x[0]
        cs = jnp.asarray(_table(h.shape[0]))
        kept, fetched = [], []
        for n in range(layers):
            wq, wk, wv, wo, wg, wu, wd = (w[n] for w in weights)
            wq, wk, wv = gather(wq, wk, wv)
            wo, = gather(wo)
            wg, wu = gather(wg, wu)
            wd, = gather(wd)
            q, k, v_ = qkv(h, cs, wq, wk, wv)
            o, lse = attend(q, k, v_)
            h1, h2, g, u = ffn(o, h, wo, wg, wu, wd)
            kept.append((h, q, k, v_, o, lse, h1, g, u))
            fetched.append((wq, wk, wv, wo, wg, wu, wd))
            h = h2
        dh, mine = dy[0], [None] * layers
        for n in reversed(range(layers)):
            h, q, k, v_, o, lse, h1, g, u = kept[n]
            wq, wk, wv, wo, wg, wu, wd = fetched[n]
            dh1, do, dwo, dwg, dwu, dwd = ffn_bwd(dh, h1, g, u, o, wo, wg, wu, wd)
            gwg, gwu = scatter(dwg, dwu)
            gwd, = scatter(dwd)
            dq, dk, dv = attend_bwd(q, k, v_, do, o, lse)
            if n:
                dh, dwq, dwk, dwv = qkv_bwd(h, cs, dq, dk, dv, dh1, (wq, wk, wv))
            else:
                dwq, dwk, dwv = qkv_bwd(h, cs, dq, dk, dv)
            mine[n] = scatter(dwq, dwk, dwv, dwo) + [gwg, gwu, gwd]
        gradients = [jnp.stack([mine[n][i] for n in range(layers)]).astype(F32) for i in range(7)]
        new = [adamw(w.astype(F32), m, v, g) for w, m, v, g in zip(weights, m, v, gradients, strict=True)]
        return tuple(one[which] for which in range(3) for one in new)

    states, cut = P(("rep", "dp"), None, None), P(None, "dp", None)
    return jax.shard_map(
        step,
        mesh=mesh,
        in_specs=(states, states) + (cut,) * 21,
        out_specs=(P("rep", "dp", None),) * 21,
        check_vma=False,
    )
```

```python
import functools

import jax
import jax.numpy as jnp
import numpy as np
from jax import lax
from jax.experimental import pallas as pl
from jax.experimental.pallas import tpu as pltpu
from jax.sharding import PartitionSpec as P

NEG = -1e30
HIDDEN = 2 * NEG
LOG2E = 1.4426950408889634
LN2 = 0.6931471805599453
VMEM = 60 * 2**20
HEAD = 128
THETA = 10000
EPS = 1e-6
NAMES = ("wq", "wk", "wv", "wo", "wg", "wu", "wd")
F32, BF16 = jnp.float32, jnp.bfloat16


def _dot(a, b, ca, cb):
    return lax.dot_general(a, b, (((ca,), (cb,)), ((), ())), preferred_element_type=F32)


def _scale(wide):
    return lax.rsqrt(jnp.mean(wide * wide, -1, keepdims=True) + EPS)


def _norm_bwd(wide, scale, d_normed):
    dot = jnp.sum(d_normed * wide, -1, keepdims=True)
    return d_normed * scale - wide * (dot * scale * scale * scale * (1.0 / wide.shape[-1]))


def _table(tokens):
    half = HEAD // 2
    angle = np.arange(tokens, dtype=np.float64)[:, None] * float(THETA) ** (-np.arange(half, dtype=np.float64) / half)
    return np.concatenate([np.cos(angle), np.sin(angle)], 1).astype(np.float32)


def _turns(cs):
    first = lax.broadcasted_iota(jnp.int32, cs.shape, 1) < HEAD // 2
    other = pltpu.roll(cs, HEAD // 2, 1)
    return jnp.where(first, cs, other), jnp.where(first, -other, cs)


def _turn(t, c, s):
    heads = [t[:, i : i + HEAD] for i in range(0, t.shape[1], HEAD)]
    return jnp.concatenate([x * c + pltpu.roll(x, HEAD // 2, 1) * s for x in heads], 1)


def _whole(shape):
    return pl.BlockSpec(shape, lambda *_: (0,) * len(shape), pipeline_mode=pl.Buffered(1))


def _rows(size, width):
    return pl.BlockSpec((size, width), lambda t: (t, 0))


def _cost(flops, *arrays, exps=0):
    return pl.CostEstimate(flops=int(flops), transcendentals=int(exps), bytes_accessed=int(sum(a.size * a.dtype.itemsize for a in arrays)))


def _params(**more):
    return pltpu.CompilerParams(vmem_limit_bytes=VMEM, **more)


def _like(shape, dtype=BF16):
    return jax.ShapeDtypeStruct(shape, dtype)


MESH = pl.DeviceIdType.MESH
ANY = pl.BlockSpec(memory_space=pl.ANY)
SLOTS = 9


class _Place:
    def __init__(self, n):
        me = lax.axis_index("dp")
        self.me, self.core, self.chip = me, lax.rem(me, 2), lax.div(me, 2)
        chips = n // 2
        self.chips = chips
        self.right_chip = lax.rem(self.chip + 1, chips)
        self.left_chip = lax.rem(self.chip + chips - 1, chips)
        self.across_chip = lax.rem(self.chip + 2, chips)
        self.right, self.left, self.across = (c * 2 + self.core for c in (self.right_chip, self.left_chip, self.across_chip))
        self.partner = self.chip * 2 + 1 - self.core

    def greet(self):
        barrier = pltpu.get_barrier_semaphore()
        for peer in (self.right, self.left, self.partner):
            pl.semaphore_signal(barrier, inc=1, device_id={"dp": peer}, device_id_type=MESH)
        pl.semaphore_wait(barrier, 3)


def _halves(rows):
    return pl.ds(0, rows // 2), pl.ds(rows // 2, rows // 2)


class Gather:
    def __init__(self, n, given, schedule, in_vmem=False):
        self.n, self.given, self.schedule = n, given, schedule
        self.inputs = [a for a, _ in given]
        shapes = [(n, *a.shape[1:]) for a, _ in given]
        self.out_shape = [] if in_vmem else [_like(s) for s in shapes]
        self.scratch = [pltpu.SemaphoreType.DMA((len(given), SLOTS))] * 2 + ([pltpu.VMEM(s, BF16) for s in shapes] if in_vmem else [])

    def bind(self, ins, outs, scratch):
        self.send, self.recv = scratch[:2]
        self.src = [ref.at[layer] for ref, (_, layer) in zip(ins, self.given)]
        self.dst = outs if outs else scratch[2:]
        self.place = _Place(self.n)
        return self

    def _copy(self, i, slot):
        p, src, dst = self.place, self.src[i], self.dst[i]
        first, second = _halves(src.shape[0])
        sends = {
            0: (src, dst.at[p.me], p.right),
            1: (src, dst.at[p.me], p.left),
            2: (src, dst.at[p.me], p.partner),
            3: (dst.at[p.left, first], dst.at[p.left, first], p.right),
            4: (dst.at[p.right, second], dst.at[p.right, second], p.left),
            5: (dst.at[p.left], dst.at[p.left], p.partner),
            6: (dst.at[p.right], dst.at[p.right], p.partner),
            7: (dst.at[p.across], dst.at[p.across], p.partner),
        }
        if slot == 8:
            return pltpu.make_async_copy(src, dst.at[p.me], self.send.at[i, 8])
        a, b, to = sends[slot]
        return pltpu.make_async_remote_copy(a, b, self.send.at[i, slot], self.recv.at[i, slot], device_id={"dp": to}, device_id_type=MESH)

    def start(self, i):
        for slot in (0, 1, 2, 8):
            self._copy(i, slot).start()

    def relay(self, i):
        for arrived, on in ((0, (3, 5)), (1, (4, 6))):
            self._copy(i, arrived).wait_recv()
            for slot in on:
                self._copy(i, slot).start()

    def cross(self, i):
        self._copy(i, 3).wait_recv()
        self._copy(i, 4).wait_recv()
        self._copy(i, 7).start()

    def finish(self, i):
        for slot in (2, 5, 6, 7):
            self._copy(i, slot).wait_recv()
        for slot in range(8):
            self._copy(i, slot).wait_send()
        self._copy(i, 8).wait()

    def at(self, point):
        _run(self, point)


class Scatter:
    def __init__(self, n, grads, schedule):
        self.n, self.schedule = n, schedule
        chips = n // 2
        blocks = [(g.shape[0] // n, g.shape[1]) for g in grads]
        self.count = len(grads)
        self.inputs = [g.reshape(chips, 2, *b) for g, b in zip(grads, blocks)]
        self.out_shape = [_like(b) for b in blocks]
        self.scratch = [pltpu.SemaphoreType.DMA((self.count, SLOTS))] * 2
        for r, c in blocks:
            self.scratch += [pltpu.VMEM((chips, r, c), BF16)] * 2 + [pltpu.VMEM((r, c), BF16)] * 2 + [pltpu.VMEM((r // 2, c), BF16)] * 2

    def bind(self, ins, outs, scratch):
        self.send, self.recv = scratch[:2]
        self.ins, self.outs = ins, outs
        self.bufs = [scratch[2 + 6 * i : 8 + 6 * i] for i in range(self.count)]
        self.place = _Place(self.n)
        return self

    def _copy(self, i, slot):
        p = self.place
        own, got, from_left, from_right, mid_left, mid_right = self.bufs[i]
        first, second = _halves(from_left.shape[0])
        if slot == 7:
            return pltpu.make_async_copy(from_left, self.outs[i], self.send.at[i, 7])
        if slot == 8:
            return pltpu.make_async_copy(self.ins[i].at[:, p.core], own, self.send.at[i, 8])
        a, b, to = {
            0: (self.ins[i].at[:, 1 - p.core], got, p.partner),
            1: (own.at[p.across_chip, first], mid_left, p.right),
            2: (own.at[p.across_chip, second], mid_right, p.left),
            3: (own.at[p.right_chip, second], from_left.at[second], p.right),
            4: (own.at[p.left_chip, first], from_right.at[first], p.left),
            5: (own.at[p.right_chip, first], from_left.at[first], p.right),
            6: (own.at[p.left_chip, second], from_right.at[second], p.left),
        }[slot]
        return pltpu.make_async_remote_copy(a, b, self.send.at[i, slot], self.recv.at[i, slot], device_id={"dp": to}, device_id_type=MESH)

    def start(self, i):
        self._copy(i, 0).start()
        self._copy(i, 8).start()

    def pair(self, i):
        own, got = self.bufs[i][:2]
        self._copy(i, 8).wait()
        self._copy(i, 0).wait_recv()

        def add(j, _):
            own[j] = (own[j].astype(F32) + got[j].astype(F32)).astype(BF16)

        lax.fori_loop(0, self.place.chips, add, None)
        for slot in (1, 2, 3, 4):
            self._copy(i, slot).start()

    def mid(self, i):
        p = self.place
        own, _, _, _, mid_left, mid_right = self.bufs[i]
        first, second = _halves(own.shape[1])
        for slot, chip, half, arrived in ((1, p.right_chip, first, mid_left), (2, p.left_chip, second, mid_right)):
            self._copy(i, slot).wait_recv()
            own[chip, half] = (own[chip, half].astype(F32) + arrived[...].astype(F32)).astype(BF16)
        self._copy(i, 5).start()
        self._copy(i, 6).start()

    def final(self, i):
        own, _, from_left, from_right, _, _ = self.bufs[i]
        for slot in (3, 4, 5, 6):
            self._copy(i, slot).wait_recv()
        total = own[self.place.chip].astype(F32) + from_left[...].astype(F32) + from_right[...].astype(F32)
        from_left[...] = total.astype(BF16)
        self._copy(i, 7).start()

    def finish(self, i):
        for slot in range(7):
            self._copy(i, slot).wait_send()
        self._copy(i, 7).wait()

    def at(self, point):
        _run(self, point)


def _run(plan, point):
    for name, items in plan.schedule.get(point, ()):
        if name == "greet":
            plan.place.greet()
        for i in items:
            getattr(plan, name)(i)


class _Idle:
    inputs, out_shape, scratch, schedule = [], [], [], {}

    def bind(self, *_):
        return self

    def at(self, point):
        pass


IDLE = _Idle()


def call(kernel, plan, number, *, grid, given, in_specs, out_specs, out_shape, scratch, cost):
    sizes = [len(given), len(plan.inputs), len(out_shape), len(plan.out_shape), len(scratch), len(plan.scratch)]
    ends = [sum(sizes[:i]) for i in range(7)]

    def body(*refs):
        a, b, c, d, e, f = (refs[ends[i] : ends[i + 1]] for i in range(6))
        kernel(plan.bind(b, d, f), *a, *c, *e)

    more = dict(collective_id=number, has_side_effects=True) if plan.inputs else {}
    got = pl.pallas_call(
        body,
        grid=grid,
        in_specs=in_specs + [ANY] * sizes[1],
        out_specs=out_specs + [ANY] * sizes[3],
        out_shape=out_shape + plan.out_shape,
        scratch_shapes=scratch + plan.scratch,
        compiler_params=_params(**more),
        cost_estimate=cost,
    )(*given, *plan.inputs)
    return got[: sizes[2]], got[sizes[2] :]


def _qkv_kernel(plan, h_ref, cs_ref, *rest, early):
    if early:
        q_ref, k_ref, v_ref = rest
    else:
        wq_ref, wk_ref, wv_ref, q_ref, k_ref, v_ref = rest
    t = pl.program_id(0)
    for step in range(4):
        if step in plan.schedule:
            pl.when(t == step)(functools.partial(plan.at, step))
    if early:
        wq_ref, wk_ref, wv_ref = (ref.reshape(-1, ref.shape[2]) for ref in early_refs(plan))
    wide = h_ref[...].astype(F32)
    a = (wide * _scale(wide)).astype(BF16)
    c, s = _turns(cs_ref[...])
    for w_ref, out in ((wq_ref, q_ref), (wk_ref, k_ref)):
        x = _dot(a, w_ref[...], 1, 0).astype(BF16).astype(F32)
        out[...] = _turn(x, c, s).astype(BF16)
    v_ref[...] = _dot(a, wv_ref[...], 1, 0).astype(BF16)
    if "end" in plan.schedule:
        pl.when(t == pl.num_programs(0) - 1)(lambda: plan.at("end"))


def early_refs(plan):
    return plan.plans[0].dst


class Both:
    def __init__(self, *plans):
        self.plans = plans
        self.inputs, self.out_shape, self.scratch = (sum((getattr(p, x) for p in plans), []) for x in ("inputs", "out_shape", "scratch"))
        self.schedule = {k: True for p in plans for k in p.schedule}

    def bind(self, ins, outs, scratch):
        for p in self.plans:
            a, b, c = len(p.inputs), len(p.out_shape), len(p.scratch)
            p.bind(ins[:a], outs[:b], scratch[:c])
            ins, outs, scratch = ins[a:], outs[b:], scratch[c:]
        return self

    def at(self, point):
        for p in self.plans:
            p.at(point)


def qkv(h, cs, ws, width, plan=IDLE, number=None, tile=512):
    tokens, d = h.shape
    return call(
        functools.partial(_qkv_kernel, early=ws is None), plan, number,
        grid=(tokens // tile,),
        given=[h, cs] + list(ws or ()),
        in_specs=[_rows(tile, d), _rows(tile, HEAD)] + [_whole((d, width))] * (3 if ws else 0),
        out_specs=[_rows(tile, width)] * 3,
        out_shape=[_like((tokens, width))] * 3,
        scratch=[],
        cost=_cost(6 * tokens * d * width, h, h, h, h),
    )


def _blocks(plan, block, causal_part, diagonal):
    iq, steps = pl.program_id(0), 4
    named = {i * (i + 1) // 2 + j: (i, j) for i in range(steps) for j in range(i + 1)}

    def ahead(inside, j=None):
        for number, (i, at) in named.items():
            if number in plan.schedule and (at < i) == inside:
                pl.when((iq == i) & (j == at) if inside else iq == i)(functools.partial(plan.at, number))

    def loop(j, _):
        ahead(True, j)
        causal_part(pl.multiple_of(j * block, block))

    lax.fori_loop(0, iq, loop, None)
    ahead(False)
    diagonal()


def _triangle(keys, queries):
    return lax.broadcasted_iota(jnp.int32, (keys, queries), 1) >= lax.broadcasted_iota(jnp.int32, (keys, queries), 0)


def _attend_kernel(plan, q_ref, k_ref, v_ref, o_ref, lse_ref, top_s, mix_s, *, scale, block):
    iq = pl.program_id(0)
    if "start" in plan.schedule:
        pl.when(iq == 0)(lambda: plan.at("start"))
    heads = q_ref.shape[1] // HEAD
    e = scale * LOG2E
    lanes = [slice(i * HEAD, (i + 1) * HEAD) for i in range(heads)]
    top_s[...] = jnp.full(top_s.shape, NEG, F32)
    mix_s[...] = jnp.zeros_like(mix_s)

    def part(key, keys, query, queries, masked):
        here, cols = pl.ds(key, keys), slice(query, query + queries)
        scores = [_dot(k_ref[here, x], q_ref[cols, x], 1, 1) for x in lanes]
        ok = _triangle(keys, queries) if masked else None
        ones = jnp.ones((8, keys), BF16)
        weights, keeps = [], []
        for i, s in enumerate(scores):
            if masked:
                s = jnp.where(ok, s, HIDDEN)
            old = top_s[i : i + 1, cols]
            top = jnp.maximum(old, s.max(axis=0, keepdims=True))
            top_s[i : i + 1, cols] = top
            weights.append(jnp.exp2((s - top) * e).astype(BF16))
            keeps.append(jnp.exp2((old - top) * e))
        for i, (p, keep) in enumerate(zip(weights, keeps)):
            values = jnp.concatenate([v_ref[here, lanes[i]].T, ones], axis=0)
            mix_s[i, :, cols] = mix_s[i, :, cols] * keep + _dot(values, p, 1, 0)

    half = block // 2
    base = pl.multiple_of(iq * block, block)

    def diagonal():
        part(base, half, 0, block, True)
        part(pl.multiple_of(base + half, half), half, half, half, True)

    _blocks(plan, block, lambda key: part(key, block, 0, block, False), diagonal)
    for i, x in enumerate(lanes):
        total = mix_s[i, HEAD : HEAD + 1, :]
        o_ref[:, x] = (mix_s[i, :HEAD, :] * (1 / total)).T.astype(BF16)
        lse_ref[i : i + 1, :] = top_s[i : i + 1, :] * scale + jnp.log(total)
    if "end" in plan.schedule:
        pl.when(iq == pl.num_programs(0) - 1)(lambda: plan.at("end"))


def attend(q, k, v, plan=IDLE, number=None):
    tokens, width = q.shape
    heads, block = width // HEAD, tokens // 4
    return call(
        functools.partial(_attend_kernel, scale=HEAD**-0.5, block=block), plan, number,
        grid=(tokens // block,),
        given=[q, k, v],
        in_specs=[_rows(block, width), _whole(k.shape), _whole(v.shape)],
        out_specs=[_rows(block, width), pl.BlockSpec((heads, block), lambda t: (0, t))],
        out_shape=[_like((tokens, width)), _like((heads, tokens), F32)],
        scratch=[pltpu.VMEM((heads, block), F32), pltpu.VMEM((heads, HEAD + 8, block), F32)],
        cost=_cost(4 * heads * tokens * tokens * HEAD, q, k, v, q, exps=heads * tokens * tokens),
    )


def _ffn_kernel(plan, o_ref, h_ref, wo_ref, wg_ref, wu_ref, wd_ref, h1_ref, h2_ref, g_ref, u_ref, *, chunk):
    t = pl.program_id(0)
    for step in range(8):
        if step in plan.schedule:
            pl.when(t == step)(functools.partial(plan.at, step))
    h1 = (h_ref[...].astype(F32) + _dot(o_ref[...], wo_ref[...], 1, 0).astype(BF16).astype(F32)).astype(BF16)
    h1_ref[...] = h1
    wide = h1.astype(F32)
    b = (wide * _scale(wide)).astype(BF16)
    total = None
    for at in range(0, wg_ref.shape[1], chunk):
        here = slice(at, at + chunk)
        gate, up = _dot(b, wg_ref[:, here], 1, 0), _dot(b, wu_ref[:, here], 1, 0)
        g_ref[:, here] = gate
        u_ref[:, here] = up
        act = (gate * jax.nn.sigmoid(gate) * up).astype(BF16)
        term = _dot(act, wd_ref[here, :], 1, 0)
        total = term if total is None else total + term
    h2_ref[...] = (wide + total.astype(BF16).astype(F32)).astype(BF16)
    if "end" in plan.schedule:
        pl.when(t == pl.num_programs(0) - 1)(lambda: plan.at("end"))


def ffn(o, h, wo, wg, wu, wd, plan=IDLE, number=None, chunk=512):
    tokens, d = h.shape
    width, hidden, tile = o.shape[1], wg.shape[1], tokens // 8
    return call(
        functools.partial(_ffn_kernel, chunk=chunk), plan, number,
        grid=(tokens // tile,),
        given=[o, h, wo, wg, wu, wd],
        in_specs=[_rows(tile, width), _rows(tile, d)] + [_whole(w.shape) for w in (wo, wg, wu, wd)],
        out_specs=[_rows(tile, d)] * 2 + [_rows(tile, hidden)] * 2,
        out_shape=[_like((tokens, d))] * 2 + [_like((tokens, hidden), F32)] * 2,
        scratch=[],
        cost=_cost(2 * tokens * d * (width + 3 * hidden), o, h, h, h, wo, wg, wu, wd),
    )


def _ffn_bwd_kernel(plan, dh2_ref, h1_ref, g_ref, u_ref, o_ref, wo_ref, wg_ref, wu_ref, wd_ref,
                    dh1_ref, do_ref, dwo_ref, dwg_ref, dwu_ref, dwd_ref, awo, awg, awu, awd, *, chunk):
    t = pl.program_id(0)
    for step in range(8):
        if step in plan.schedule:
            pl.when(t == step)(functools.partial(plan.at, step))

    @pl.when(t == 0)
    def _():
        for acc in (awo, awg, awu, awd):
            acc[...] = jnp.zeros_like(acc)

    dh2 = dh2_ref[...]
    wide = h1_ref[...].astype(F32)
    scale = _scale(wide)
    b = (wide * scale).astype(BF16)
    db = None
    for at in range(0, wg_ref.shape[1], chunk):
        here = slice(at, at + chunk)
        d_act = _dot(dh2, wd_ref[here, :], 1, 1).astype(BF16).astype(F32)
        gate, up = g_ref[:, here], u_ref[:, here]
        sig = jax.nn.sigmoid(gate)
        silu = gate * sig
        act = (silu * up).astype(BF16)
        d_up = (d_act * silu).astype(BF16)
        d_gate = (d_act * up * (sig + silu * (1 - sig))).astype(BF16)
        term = _dot(d_gate, wg_ref[:, here], 1, 1) + _dot(d_up, wu_ref[:, here], 1, 1)
        db = term if db is None else db + term
        awd[here, :] += _dot(act, dh2, 0, 0)
        awg[:, here] += _dot(b, d_gate, 0, 0)
        awu[:, here] += _dot(b, d_up, 0, 0)
    db = db.astype(BF16).astype(F32)
    dh1 = (dh2.astype(F32) + _norm_bwd(wide, scale, db).astype(BF16).astype(F32)).astype(BF16)
    dh1_ref[...] = dh1
    do_ref[...] = _dot(dh1, wo_ref[...], 1, 1).astype(BF16)
    awo[...] += _dot(o_ref[...], dh1, 0, 0)

    @pl.when(t == pl.num_programs(0) - 1)
    def _():
        for out, acc in ((dwo_ref, awo), (dwg_ref, awg), (dwu_ref, awu), (dwd_ref, awd)):
            out[...] = acc[...].astype(BF16)
        plan.at("end")


def ffn_bwd(dh2, h1, g, u, o, wo, wg, wu, wd, plan=IDLE, number=None, chunk=512):
    tokens, d = h1.shape
    width, hidden, tile = o.shape[1], wg.shape[1], tokens // 8
    ws = (wo, wg, wu, wd)
    return call(
        functools.partial(_ffn_bwd_kernel, chunk=chunk), plan, number,
        grid=(tokens // tile,),
        given=[dh2, h1, g, u, o, *ws],
        in_specs=[_rows(tile, d), _rows(tile, d), _rows(tile, hidden), _rows(tile, hidden), _rows(tile, width)] + [_whole(w.shape) for w in ws],
        out_specs=[_rows(tile, d), _rows(tile, width)] + [_whole(w.shape) for w in ws],
        out_shape=[_like((tokens, d)), _like((tokens, width))] + [_like(w.shape) for w in ws],
        scratch=[pltpu.VMEM(w.shape, F32) for w in ws],
        cost=_cost(4 * tokens * d * (width + 3 * hidden), g, u, h1, h1, h1, *ws, *ws),
    )


def _attend_bwd_kernel(plan, q_ref, k_ref, v_ref, do_ref, o_ref, lse_ref, dq_ref, dk_ref, dv_ref, dq_s, dk_s, dv_s, *, scale, block):
    iq = pl.program_id(0)
    if "start" in plan.schedule:
        pl.when(iq == 0)(lambda: plan.at("start"))
    heads = q_ref.shape[1] // HEAD
    e = scale * LOG2E
    lanes = [slice(i * HEAD, (i + 1) * HEAD) for i in range(heads)]

    @pl.when(iq == 0)
    def _():
        dk_s[...] = jnp.zeros_like(dk_s)
        dv_s[...] = jnp.zeros_like(dv_s)

    dq_s[...] = jnp.zeros_like(dq_s)
    lses = [lse_ref[i : i + 1, :] * LOG2E for i in range(heads)]
    deltas = [(do_ref[:, x].astype(F32) * o_ref[:, x].astype(F32)).T.sum(axis=0, keepdims=True) for x in lanes]

    def part(key, keys, query, queries, masked):
        here, cols = pl.ds(key, keys), slice(query, query + queries)
        scores = [_dot(k_ref[here, x], q_ref[cols, x], 1, 1) for x in lanes]
        dps = [_dot(v_ref[here, x], do_ref[cols, x], 1, 1) for x in lanes]
        ok = _triangle(keys, queries) if masked else None
        for i, x in enumerate(lanes):
            p = jnp.exp2(scores[i] * e - lses[i][:, cols])
            if masked:
                p = jnp.where(ok, p, 0.0)
            ds = (p * (dps[i] - deltas[i][:, cols])).astype(BF16)
            dv_s[here, x] += _dot(p.astype(BF16), do_ref[cols, x], 1, 0)
            dk_s[here, x] += _dot(ds, q_ref[cols, x], 1, 0)
            dq_s[i, :, cols] += _dot(k_ref[here, x].T, ds, 1, 0)

    half = block // 2
    base = pl.multiple_of(iq * block, block)

    def diagonal():
        part(base, half, 0, block, True)
        part(pl.multiple_of(base + half, half), half, half, half, True)

    _blocks(plan, block, lambda key: part(key, block, 0, block, False), diagonal)
    for i, x in enumerate(lanes):
        dq_ref[:, x] = (dq_s[i] * scale).T.astype(BF16)

    @pl.when(iq == pl.num_programs(0) - 1)
    def _():
        dk_ref[...] = (dk_s[...] * scale).astype(BF16)
        dv_ref[...] = dv_s[...].astype(BF16)
        plan.at("end")


def attend_bwd(q, k, v, do, o, lse, plan=IDLE, number=None):
    tokens, width = q.shape
    heads, block = width // HEAD, tokens // 4
    return call(
        functools.partial(_attend_bwd_kernel, scale=HEAD**-0.5, block=block), plan, number,
        grid=(tokens // block,),
        given=[q, k, v, do, o, lse],
        in_specs=[_rows(block, width), _whole(k.shape), _whole(v.shape), _rows(block, width), _rows(block, width),
                  pl.BlockSpec((heads, block), lambda t: (0, t))],
        out_specs=[_rows(block, width), _whole(k.shape), _whole(v.shape)],
        out_shape=[_like((tokens, width))] * 3,
        scratch=[pltpu.VMEM((heads, HEAD, block), F32), pltpu.VMEM(k.shape, F32), pltpu.VMEM(v.shape, F32)],
        cost=_cost(10 * heads * tokens * tokens * HEAD, q, k, v, do, o, q, k, v, exps=heads * tokens * tokens),
    )


def _qkv_bwd_kernel(h_ref, cs_ref, dq_ref, dk_ref, dv_ref, *rest, inner):
    if inner:
        dh1_ref, wq_ref, wk_ref, wv_ref, dh_ref, dwq_ref, dwk_ref, dwv_ref, *accs = rest
    else:
        dwq_ref, dwk_ref, dwv_ref, *accs = rest
    t = pl.program_id(0)

    @pl.when(t == 0)
    def _():
        for acc in accs:
            acc[...] = jnp.zeros_like(acc)

    wide = h_ref[...].astype(F32)
    scale = _scale(wide)
    a = (wide * scale).astype(BF16)
    c, s = _turns(cs_ref[...])
    grads = [_turn(ref[...].astype(F32), c, -s).astype(BF16) for ref in (dq_ref, dk_ref)] + [dv_ref[...]]
    for acc, g in zip(accs, grads):
        acc[...] += _dot(a, g, 0, 0)
    if inner:
        da = sum(_dot(g, w[...], 1, 1) for g, w in zip(grads, (wq_ref, wk_ref, wv_ref)))
        da = da.astype(BF16).astype(F32)
        dh_ref[...] = (dh1_ref[...].astype(F32) + _norm_bwd(wide, scale, da).astype(BF16).astype(F32)).astype(BF16)

    @pl.when(t == pl.num_programs(0) - 1)
    def _():
        for out, acc in zip((dwq_ref, dwk_ref, dwv_ref), accs):
            out[...] = acc[...].astype(BF16)


def qkv_bwd(h, cs, dq, dk, dv, dh1=None, ws=None, tile=512):
    tokens, d = h.shape
    width = dq.shape[1]
    inner = dh1 is not None
    given = [h, cs, dq, dk, dv] + ([dh1, *ws] if inner else [])
    specs = [_rows(tile, d), _rows(tile, HEAD)] + [_rows(tile, width)] * 3 + ([_rows(tile, d)] + [_whole((d, width))] * 3 if inner else [])
    return pl.pallas_call(
        functools.partial(_qkv_bwd_kernel, inner=inner),
        grid=(tokens // tile,),
        in_specs=specs,
        out_specs=([_rows(tile, d)] if inner else []) + [_whole((d, width))] * 3,
        out_shape=([_like((tokens, d))] if inner else []) + [_like((d, width))] * 3,
        scratch_shapes=[pltpu.VMEM((d, width), F32)] * 3,
        compiler_params=_params(),
        cost_estimate=_cost((12 if inner else 6) * tokens * d * width, *given),
    )(*given)


def adamw(w, m, v, g):
    m = 0.9 * m + 0.1 * g
    v = 0.95 * v + 0.05 * g * g
    step = m * lax.rsqrt(v + 1e-8) + 0.1 * w
    return (w - 0.02 * step).astype(BF16), m, v


def _tail_kernel(plan):
    for point in range(4):
        plan.at(point)


def solution(mesh):
    n = mesh.shape["dp"]

    def flat(w):
        return w.reshape(-1, w.shape[2])

    def step(x, dy, *arrays):
        weights, m, v = (arrays[i : i + 7] for i in (0, 7, 14))
        wq, wk, wv, wo, wg, wu, wd = weights
        layers, width = wq.shape[0], wq.shape[2]
        h = x[0]
        cs = jnp.asarray(_table(h.shape[0]))
        both = Both(
            Gather(n, [(wq, 0), (wk, 0), (wv, 0)],
                   {0: [("greet", ()), ("start", (0, 1, 2))]}, in_vmem=True),
            Gather(n, [(wo, 0), (wg, 0)],
                   {0: [("start", (0, 1))], 3: [("relay", (0, 1))], "end": [("cross", (0, 1)), ("finish", (0, 1))]}),
        )
        first = both.plans[0]
        second = both.plans[1]
        first.schedule[0] = [("greet", ()), ("start", (0, 1, 2))]
        second.schedule[0] = [("start", (0, 1))]

        class Late:
            inputs, out_shape, scratch = [], [], []
            schedule = {0: True}

            def bind(self, *_):
                return self

            def at(self, point):
                if point == 0:
                    for name in ("relay", "cross", "finish"):
                        for i in range(3):
                            getattr(first, name)(i)

        both = Both(first, second, Late())
        at_start = qkv(h, cs, None, width, both, 1)
        gathered = {}
        kept = []
        gathered["wo", 0], gathered["wg", 0] = at_start[1]
        in_attention = {"start": [("greet", ()), ("start", (0, 1))], 4: [("relay", (0,))], 7: [("relay", (1,)), ("cross", (0,))],
                        "end": [("cross", (1,)), ("finish", (0, 1))]}
        for i in range(layers):
            if i == 0:
                q, k, v_ = at_start[0]
                (o, lse), (gathered["wu", 0], gathered["wd", 0]) = attend(q, k, v_, Gather(n, [(wu, 0), (wd, 0)], in_attention), 2)
            else:
                (q, k, v_), _ = qkv(h, cs, [flat(gathered[name, i]) for name in ("wq", "wk", "wv")], width)
                (o, lse), (gathered["wg", i], gathered["wu", i]) = attend(q, k, v_, Gather(n, [(wg, i), (wu, i)], in_attention), 4 + 2 * i)
            plan = IDLE
            if i + 1 < layers:
                plan = Gather(n, [(w, i + 1) for w in (wq, wk, wv, wo, wd)],
                              {0: [("greet", ()), ("start", range(5))], 3: [("relay", range(4))], 5: [("relay", (4,)), ("cross", range(4))],
                               "end": [("cross", (4,)), ("finish", range(5))]})
            (h1, h2, g, u), got = ffn(o, h, *(flat(gathered[name, i]) for name in ("wo", "wg", "wu", "wd")), plan, 3 + 2 * i)
            for name, one in zip(("wq", "wk", "wv", "wo", "wd"), got):
                gathered[name, i + 1] = one
            kept.append((h, q, k, v_, o, lse, h1, g, u))
            h = h2
        dh, mine = dy[0], {}
        waiting, names = [], []
        for i in reversed(range(layers)):
            h, q, k, v_, o, lse, h1, g, u = kept[i]
            plan = IDLE
            if waiting:
                every = range(len(waiting))
                plan = Scatter(n, waiting, {0: [("greet", ()), ("start", every)], 1: [("pair", every)], 3: [("mid", every)],
                                            5: [("final", every)], "end": [("finish", every)]})
            (dh1, do, dwo, dwg, dwu, dwd), got = ffn_bwd(dh, h1, g, u, o, *(flat(gathered[name, i]) for name in ("wo", "wg", "wu", "wd")),
                                                         plan, 20 + 3 * i)
            mine.update(zip(names, got))
            plan = Scatter(n, [dwo, dwg, dwu, dwd], {"start": [("greet", ()), ("start", range(4))], 1: [("pair", (0, 1))], 2: [("pair", (2, 3))],
                                                     3: [("mid", (0, 1))], 5: [("mid", (2,))], 6: [("mid", (3,))], 7: [("final", (0,))],
                                                     8: [("final", (1,))], 9: [("final", (2,))], "end": [("final", (3,)), ("finish", range(4))]})
            (dq, dk, dv), got = attend_bwd(q, k, v_, do, o, lse, plan, 21 + 3 * i)
            mine.update(zip([(name, i) for name in ("wo", "wg", "wu", "wd")], got))
            if i:
                dh, *waiting = qkv_bwd(h, cs, dq, dk, dv, dh1, [flat(gathered[name, i]) for name in ("wq", "wk", "wv")])
            else:
                waiting = qkv_bwd(h, cs, dq, dk, dv)
            names = [(name, i) for name in ("wq", "wk", "wv")]
        every = range(len(waiting))
        plan = Scatter(n, waiting, {0: [("greet", ()), ("start", every)], 1: [("pair", every)], 2: [("mid", every)],
                                    3: [("final", every), ("finish", every)]})
        _, got = call(_tail_kernel, plan, 40, grid=(), given=[], in_specs=[], out_specs=[], out_shape=[], scratch=[], cost=None)
        mine.update(zip(names, got))
        gradients = [jnp.stack([mine[name, i] for i in range(layers)]).astype(F32) for name in NAMES]
        new = [adamw(w.astype(F32), m, v, g) for w, m, v, g in zip(weights, m, v, gradients, strict=True)]
        return tuple(one[which] for which in range(3) for one in new)

    states, cut = P(("rep", "dp"), None, None), P(None, "dp", None)
    return jax.shard_map(
        step,
        mesh=mesh,
        in_specs=(states, states) + (cut,) * 21,
        out_specs=(P("rep", "dp", None),) * 21,
        check_vma=False,
    )
```

```python
import functools

import jax
import jax.numpy as jnp
import numpy as np
from jax import lax
from jax.experimental import pallas as pl
from jax.experimental.pallas import tpu as pltpu
from jax.sharding import PartitionSpec as P

NEG = -1e30
HIDDEN = 2 * NEG
LOG2E = 1.4426950408889634
LN2 = 0.6931471805599453
VMEM = 60 * 2**20
HEAD = 128
THETA = 10000
EPS = 1e-6
NAMES = ("wq", "wk", "wv", "wo", "wg", "wu", "wd")
F32, BF16 = jnp.float32, jnp.bfloat16


def _dot(a, b, ca, cb):
    return lax.dot_general(a, b, (((ca,), (cb,)), ((), ())), preferred_element_type=F32)


def _scale(wide):
    return lax.rsqrt(jnp.mean(wide * wide, -1, keepdims=True) + EPS)


def _norm_bwd(wide, scale, d_normed):
    dot = jnp.sum(d_normed * wide, -1, keepdims=True)
    return d_normed * scale - wide * (dot * scale * scale * scale * (1.0 / wide.shape[-1]))


def _table(tokens):
    half = HEAD // 2
    angle = np.arange(tokens, dtype=np.float64)[:, None] * float(THETA) ** (-np.arange(half, dtype=np.float64) / half)
    return np.concatenate([np.cos(angle), np.sin(angle)], 1).astype(np.float32)


def _turns(cs):
    first = lax.broadcasted_iota(jnp.int32, cs.shape, 1) < HEAD // 2
    other = pltpu.roll(cs, HEAD // 2, 1)
    return jnp.where(first, cs, other), jnp.where(first, -other, cs)


def _turn(t, c, s):
    heads = [t[:, i : i + HEAD] for i in range(0, t.shape[1], HEAD)]
    return jnp.concatenate([x * c + pltpu.roll(x, HEAD // 2, 1) * s for x in heads], 1)


def _whole(shape):
    return pl.BlockSpec(shape, lambda *_: (0,) * len(shape), pipeline_mode=pl.Buffered(1))


def _rows(size, width):
    return pl.BlockSpec((size, width), lambda t: (t, 0))


def _cost(flops, *arrays, exps=0):
    return pl.CostEstimate(flops=int(flops), transcendentals=int(exps), bytes_accessed=int(sum(a.size * a.dtype.itemsize for a in arrays)))


def _params(**more):
    return pltpu.CompilerParams(vmem_limit_bytes=VMEM, **more)


def _like(shape, dtype=BF16):
    return jax.ShapeDtypeStruct(shape, dtype)


MESH = pl.DeviceIdType.MESH
ANY = pl.BlockSpec(memory_space=pl.ANY)
SLOTS = 9


class _Place:
    def __init__(self, n):
        me = lax.axis_index("dp")
        self.me, self.core, self.chip = me, lax.rem(me, 2), lax.div(me, 2)
        chips = n // 2
        self.chips = chips
        self.right_chip = lax.rem(self.chip + 1, chips)
        self.left_chip = lax.rem(self.chip + chips - 1, chips)
        self.across_chip = lax.rem(self.chip + 2, chips)
        self.right, self.left, self.across = (c * 2 + self.core for c in (self.right_chip, self.left_chip, self.across_chip))
        self.partner = self.chip * 2 + 1 - self.core

    def greet(self):
        barrier = pltpu.get_barrier_semaphore()
        for peer in (self.right, self.left, self.partner):
            pl.semaphore_signal(barrier, inc=1, device_id={"dp": peer}, device_id_type=MESH)
        pl.semaphore_wait(barrier, 3)


def _halves(rows):
    return pl.ds(0, rows // 2), pl.ds(rows // 2, rows // 2)


class Gather:
    def __init__(self, n, given, schedule, in_vmem=False):
        self.n, self.given, self.schedule = n, given, schedule
        self.inputs = [a for a, _ in given]
        shapes = [(n, *a.shape[1:]) for a, _ in given]
        self.out_shape = [] if in_vmem else [_like(s) for s in shapes]
        self.scratch = [pltpu.SemaphoreType.DMA((len(given), SLOTS))] * 2 + [pltpu.VMEM(s if in_vmem else s[1:], BF16) for s in shapes]

    def bind(self, ins, outs, scratch):
        self.send, self.recv = scratch[:2]
        self.src = [ref.at[layer] for ref, (_, layer) in zip(ins, self.given)]
        self.dst, self.own = (outs, scratch[2:]) if outs else (scratch[2:], None)
        self.place = _Place(self.n)
        return self

    def _copy(self, i, slot):
        p, src, dst = self.place, self.src[i], self.dst[i]
        first, second = _halves(src.shape[0])
        sends = {
            0: (src, dst.at[p.me], p.right),
            1: (src, dst.at[p.me], p.left),
            2: (src, dst.at[p.me], p.partner),
            3: (dst.at[p.left, first], dst.at[p.left, first], p.right),
            4: (dst.at[p.right, second], dst.at[p.right, second], p.left),
            5: (dst.at[p.left], dst.at[p.left], p.partner),
            6: (dst.at[p.right], dst.at[p.right], p.partner),
            7: (dst.at[p.across], dst.at[p.across], p.partner),
        }
        if slot == 8:
            return pltpu.make_async_copy(src, self.own[i] if self.own else dst.at[p.me], self.send.at[i, 8])
        if slot == 9:
            return pltpu.make_async_copy(self.own[i], dst.at[p.me], self.recv.at[i, 8])
        a, b, to = sends[slot]
        return pltpu.make_async_remote_copy(a, b, self.send.at[i, slot], self.recv.at[i, slot], device_id={"dp": to}, device_id_type=MESH)

    def start(self, i):
        for slot in (0, 1, 2, 8):
            self._copy(i, slot).start()

    def relay(self, i):
        for arrived, on in ((0, (3, 5)), (1, (4, 6))):
            self._copy(i, arrived).wait_recv()
            for slot in on:
                self._copy(i, slot).start()
        if self.own:
            self._copy(i, 8).wait()
            self._copy(i, 9).start()

    def cross(self, i):
        self._copy(i, 3).wait_recv()
        self._copy(i, 4).wait_recv()
        self._copy(i, 7).start()

    def finish(self, i):
        for slot in (2, 5, 6, 7):
            self._copy(i, slot).wait_recv()
        for slot in range(8):
            self._copy(i, slot).wait_send()
        self._copy(i, 9 if self.own else 8).wait()

    def at(self, point):
        _run(self, point)


class Scatter:
    def __init__(self, n, grads, schedule):
        self.n, self.schedule = n, schedule
        chips = n // 2
        blocks = [(g.shape[0] // n, g.shape[1]) for g in grads]
        self.count = len(grads)
        self.inputs = [g.reshape(chips, 2, *b) for g, b in zip(grads, blocks)]
        self.out_shape = [_like(b) for b in blocks]
        self.scratch = [pltpu.SemaphoreType.DMA((self.count, SLOTS))] * 2
        for r, c in blocks:
            self.scratch += [pltpu.VMEM((chips, r, c), BF16)] * 2 + [pltpu.VMEM((r, c), BF16)] * 2 + [pltpu.VMEM((r // 2, c), BF16)] * 2

    def bind(self, ins, outs, scratch):
        self.send, self.recv = scratch[:2]
        self.ins, self.outs = ins, outs
        self.bufs = [scratch[2 + 6 * i : 8 + 6 * i] for i in range(self.count)]
        self.place = _Place(self.n)
        return self

    def _copy(self, i, slot):
        p = self.place
        own, got, from_left, from_right, mid_left, mid_right = self.bufs[i]
        first, second = _halves(from_left.shape[0])
        if slot == 7:
            return pltpu.make_async_copy(from_left, self.outs[i], self.send.at[i, 7])
        if slot == 8:
            return pltpu.make_async_copy(self.ins[i].at[:, p.core], own, self.send.at[i, 8])
        a, b, to = {
            0: (self.ins[i].at[:, 1 - p.core], got, p.partner),
            1: (own.at[p.across_chip, first], mid_left, p.right),
            2: (own.at[p.across_chip, second], mid_right, p.left),
            3: (own.at[p.right_chip, second], from_left.at[second], p.right),
            4: (own.at[p.left_chip, first], from_right.at[first], p.left),
            5: (own.at[p.right_chip, first], from_left.at[first], p.right),
            6: (own.at[p.left_chip, second], from_right.at[second], p.left),
        }[slot]
        return pltpu.make_async_remote_copy(a, b, self.send.at[i, slot], self.recv.at[i, slot], device_id={"dp": to}, device_id_type=MESH)

    def start(self, i):
        self._copy(i, 0).start()
        self._copy(i, 8).start()

    def pair(self, i):
        own, got = self.bufs[i][:2]
        self._copy(i, 8).wait()
        self._copy(i, 0).wait_recv()

        def add(j, _):
            own[j] = (own[j].astype(F32) + got[j].astype(F32)).astype(BF16)

        lax.fori_loop(0, self.place.chips, add, None)
        self._copy(i, 1).start()
        self._copy(i, 2).start()

    def mid(self, i):
        p = self.place
        own, _, _, _, mid_left, mid_right = self.bufs[i]
        first, second = _halves(own.shape[1])
        for slot, chip, half, arrived in ((1, p.right_chip, first, mid_left), (2, p.left_chip, second, mid_right)):
            self._copy(i, slot).wait_recv()
            own[chip, half] = (own[chip, half].astype(F32) + arrived[...].astype(F32)).astype(BF16)
        for slot in (5, 6, 3, 4):
            self._copy(i, slot).start()

    def final(self, i):
        own, _, from_left, from_right, _, _ = self.bufs[i]
        for slot in (3, 4, 5, 6):
            self._copy(i, slot).wait_recv()
        total = own[self.place.chip].astype(F32) + from_left[...].astype(F32) + from_right[...].astype(F32)
        from_left[...] = total.astype(BF16)
        self._copy(i, 7).start()

    def finish(self, i):
        for slot in range(7):
            self._copy(i, slot).wait_send()
        self._copy(i, 7).wait()

    def at(self, point):
        _run(self, point)


def _run(plan, point):
    for name, items in plan.schedule.get(point, ()):
        _act(plan, name, items)


def _act(plan, name, items):
    if name == "greet":
        plan.place.greet()
    for i in items:
        getattr(plan, name)(i)


def _point(plan, t, steps, *rest):
    for step in range(steps):
        key = (step, *rest) if rest else step
        if key in plan.schedule:
            pl.when(t == step)(functools.partial(plan.at, key))


class _Idle:
    inputs, out_shape, scratch, schedule = [], [], [], {}

    def bind(self, *_):
        return self

    def at(self, point):
        pass


IDLE = _Idle()


def call(kernel, plan, number, *, grid, given, in_specs, out_specs, out_shape, scratch, cost):
    sizes = [len(given), len(plan.inputs), len(out_shape), len(plan.out_shape), len(scratch), len(plan.scratch)]
    ends = [sum(sizes[:i]) for i in range(7)]

    def body(*refs):
        a, b, c, d, e, f = (refs[ends[i] : ends[i + 1]] for i in range(6))
        kernel(plan.bind(b, d, f), *a, *c, *e)

    more = dict(collective_id=number, has_side_effects=True) if plan.inputs else {}
    got = pl.pallas_call(
        body,
        grid=grid,
        in_specs=in_specs + [ANY] * sizes[1],
        out_specs=out_specs + [ANY] * sizes[3],
        out_shape=out_shape + plan.out_shape,
        scratch_shapes=scratch + plan.scratch,
        compiler_params=_params(**more),
        cost_estimate=cost,
    )(*given, *plan.inputs)
    return got[: sizes[2]], got[sizes[2] :]


class Both:
    def __init__(self, plans, schedule):
        self.plans, self.schedule = plans, schedule
        self.inputs, self.out_shape, self.scratch = (sum((getattr(p, x) for p in plans), []) for x in ("inputs", "out_shape", "scratch"))

    def bind(self, ins, outs, scratch):
        for p in self.plans:
            a, b, c = len(p.inputs), len(p.out_shape), len(p.scratch)
            p.bind(ins[:a], outs[:b], scratch[:c])
            ins, outs, scratch = ins[a:], outs[b:], scratch[c:]
        return self

    def at(self, point):
        for number, name, items in self.schedule.get(point, ()):
            _act(self.plans[number], name, items)


def _blocks(plan, block, causal_part, diagonal):
    iq, steps = pl.program_id(0), 4
    named = {i * (i + 1) // 2 + j: (i, j) for i in range(steps) for j in range(i + 1)}

    def ahead(inside, j=None):
        for number, (i, at) in named.items():
            if number in plan.schedule and (at < i) == inside:
                pl.when((iq == i) & (j == at) if inside else iq == i)(functools.partial(plan.at, number))

    def loop(j, _):
        ahead(True, j)
        causal_part(pl.multiple_of(j * block, block))

    lax.fori_loop(0, iq, loop, None)
    ahead(False)
    diagonal()


def _triangle(keys, queries):
    return lax.broadcasted_iota(jnp.int32, (keys, queries), 1) >= lax.broadcasted_iota(jnp.int32, (keys, queries), 0)


def _attend_kernel(plan, h_ref, cs_ref, *rest, scale, block, early):
    iq = pl.program_id(0)
    if "start" in plan.schedule:
        pl.when(iq == 0)(lambda: plan.at("start"))
    if early:
        wq_ref, wk_ref, wv_ref = (ref.reshape(-1, ref.shape[2]) for ref in plan.plans[0].dst)
    else:
        wq_ref, wk_ref, wv_ref, *rest = rest
    q_ref, k_out, v_out, o_ref, lse_ref, k_ref, v_ref, top_s, mix_s = rest
    here = pl.ds(pl.multiple_of(iq * block, block), block)
    wide = h_ref[...].astype(F32)
    a = (wide * _scale(wide)).astype(BF16)
    c, s = _turns(cs_ref[...])
    v = _dot(a, wv_ref[...], 1, 0).astype(BF16)
    v_out[...] = v
    v_ref[here, :] = v
    q_ref[...] = _turn(_dot(a, wq_ref[...], 1, 0).astype(BF16).astype(F32), c, s).astype(BF16)
    k = _turn(_dot(a, wk_ref[...], 1, 0).astype(BF16).astype(F32), c, s).astype(BF16)
    k_out[...] = k
    k_ref[here, :] = k
    heads = q_ref.shape[1] // HEAD
    e = scale * LOG2E
    lanes = [slice(i * HEAD, (i + 1) * HEAD) for i in range(heads)]
    top_s[...] = jnp.full(top_s.shape, NEG, F32)
    mix_s[...] = jnp.zeros_like(mix_s)

    def part(key, keys, query, queries, masked):
        here, cols = pl.ds(key, keys), slice(query, query + queries)
        scores = [_dot(k_ref[here, x], q_ref[cols, x], 1, 1) for x in lanes]
        ok = _triangle(keys, queries) if masked else None
        ones = jnp.ones((8, keys), BF16)
        weights, keeps = [], []
        for i, s in enumerate(scores):
            if masked:
                s = jnp.where(ok, s, HIDDEN)
            old = top_s[i : i + 1, cols]
            top = jnp.maximum(old, s.max(axis=0, keepdims=True))
            top_s[i : i + 1, cols] = top
            weights.append(jnp.exp2((s - top) * e).astype(BF16))
            keeps.append(jnp.exp2((old - top) * e))
        for i, (p, keep) in enumerate(zip(weights, keeps)):
            values = jnp.concatenate([v_ref[here, lanes[i]].T, ones], axis=0)
            mix_s[i, :, cols] = mix_s[i, :, cols] * keep + _dot(values, p, 1, 0)

    half = block // 2
    base = pl.multiple_of(iq * block, block)

    def diagonal():
        part(base, half, 0, block, True)
        part(pl.multiple_of(base + half, half), half, half, half, True)

    _blocks(plan, block, lambda key: part(key, block, 0, block, False), diagonal)
    for i, x in enumerate(lanes):
        total = mix_s[i, HEAD : HEAD + 1, :]
        o_ref[:, x] = (mix_s[i, :HEAD, :] * (1 / total)).T.astype(BF16)
        lse_ref[i : i + 1, :] = top_s[i : i + 1, :] * scale + jnp.log(total)
    if "end" in plan.schedule:
        pl.when(iq == pl.num_programs(0) - 1)(lambda: plan.at("end"))


def attend(h, cs, ws, width, plan=IDLE, number=None):
    tokens, d = h.shape
    heads, block = width // HEAD, tokens // 4
    early = ws is None
    return call(
        functools.partial(_attend_kernel, scale=HEAD**-0.5, block=block, early=early), plan, number,
        grid=(tokens // block,),
        given=[h, cs] + list(ws or ()),
        in_specs=[_rows(block, d), _rows(block, HEAD)] + [_whole((d, width))] * (0 if early else 3),
        out_specs=[_rows(block, width)] * 4 + [pl.BlockSpec((heads, block), lambda t: (0, t))],
        out_shape=[_like((tokens, width))] * 4 + [_like((heads, tokens), F32)],
        scratch=[pltpu.VMEM((tokens, width), BF16)] * 2 + [pltpu.VMEM((heads, block), F32), pltpu.VMEM((heads, HEAD + 8, block), F32)],
        cost=_cost(4 * heads * tokens * tokens * HEAD + 6 * tokens * d * width, h, h, h, h, h, exps=heads * tokens * tokens),
    )


def _ffn_kernel(plan, o_ref, h_ref, wo_ref, wg_ref, wu_ref, wd_ref, h1_ref, h2_ref, g_ref, u_ref, *, chunk):
    t = pl.program_id(0)
    _point(plan, t, 4, 0)
    h1 = (h_ref[...].astype(F32) + _dot(o_ref[...], wo_ref[...], 1, 0).astype(BF16).astype(F32)).astype(BF16)
    h1_ref[...] = h1
    wide = h1.astype(F32)
    b = (wide * _scale(wide)).astype(BF16)
    total = None
    for at in range(0, wg_ref.shape[1], chunk):
        here = slice(at, at + chunk)
        if at:
            _point(plan, t, 4, at // chunk)
        gate, up = _dot(b, wg_ref[:, here], 1, 0), _dot(b, wu_ref[:, here], 1, 0)
        g_ref[:, here] = gate
        u_ref[:, here] = up
        act = (gate * jax.nn.sigmoid(gate) * up).astype(BF16)
        term = _dot(act, wd_ref[here, :], 1, 0)
        total = term if total is None else total + term
    h2_ref[...] = (wide + total.astype(BF16).astype(F32)).astype(BF16)
    if "end" in plan.schedule:
        pl.when(t == pl.num_programs(0) - 1)(lambda: plan.at("end"))


def ffn(o, h, wo, wg, wu, wd, plan=IDLE, number=None, chunk=512, parts=4):
    tokens, d = h.shape
    width, hidden, tile = o.shape[1], wg.shape[1], tokens // parts
    return call(
        functools.partial(_ffn_kernel, chunk=chunk), plan, number,
        grid=(tokens // tile,),
        given=[o, h, wo, wg, wu, wd],
        in_specs=[_rows(tile, width), _rows(tile, d)] + [_whole(w.shape) for w in (wo, wg, wu, wd)],
        out_specs=[_rows(tile, d)] * 2 + [_rows(tile, hidden)] * 2,
        out_shape=[_like((tokens, d))] * 2 + [_like((tokens, hidden), F32)] * 2,
        scratch=[],
        cost=_cost(2 * tokens * d * (width + 3 * hidden), o, h, h, h, wo, wg, wu, wd),
    )


def _ffn_bwd_kernel(plan, dh2_ref, o_ref, *rest, chunk, last):
    if last:
        h_ref, *rest = rest
    else:
        h1_ref, g_ref, u_ref, *rest = rest
    wo_ref, wg_ref, wu_ref, wd_ref, dh1_ref, do_ref, dwo_ref, dwg_ref, dwu_ref, dwd_ref, awo, awg, awu, awd = rest
    t = pl.program_id(0)
    _point(plan, t, 4, 0)

    @pl.when(t == 0)
    def _():
        for acc in (awo, awg, awu, awd):
            acc[...] = jnp.zeros_like(acc)

    dh2, o = dh2_ref[...], o_ref[...]
    if last:
        wide = (h_ref[...].astype(F32) + _dot(o, wo_ref[...], 1, 0).astype(BF16).astype(F32)).astype(BF16).astype(F32)
    else:
        wide = h1_ref[...].astype(F32)
    scale = _scale(wide)
    b = (wide * scale).astype(BF16)
    b_t = b.T
    db = None
    for at in range(0, wg_ref.shape[1], chunk):
        here = slice(at, at + chunk)
        if at:
            _point(plan, t, 4, at // chunk)
        d_act = _dot(dh2, wd_ref[here, :], 1, 1).astype(BF16).astype(F32)
        if last:
            gate, up = _dot(b, wg_ref[:, here], 1, 0), _dot(b, wu_ref[:, here], 1, 0)
        else:
            gate, up = g_ref[:, here], u_ref[:, here]
        sig = jax.nn.sigmoid(gate)
        silu = gate * sig
        act = (silu * up).astype(BF16)
        d_up = (d_act * silu).astype(BF16)
        d_gate = (d_act * up * (sig + silu * (1 - sig))).astype(BF16)
        term = _dot(d_gate, wg_ref[:, here], 1, 1) + _dot(d_up, wu_ref[:, here], 1, 1)
        db = term if db is None else db + term
        awd[here, :] += _dot(act.T, dh2, 1, 0)
        awg[:, here] += _dot(b_t, d_gate, 1, 0)
        awu[:, here] += _dot(b_t, d_up, 1, 0)
    db = db.astype(BF16).astype(F32)
    dh1 = (dh2.astype(F32) + _norm_bwd(wide, scale, db).astype(BF16).astype(F32)).astype(BF16)
    dh1_ref[...] = dh1
    do_ref[...] = _dot(dh1, wo_ref[...], 1, 1).astype(BF16)
    awo[...] += _dot(o.T, dh1, 1, 0)

    @pl.when(t == pl.num_programs(0) - 1)
    def _():
        for out, acc in ((dwo_ref, awo), (dwg_ref, awg), (dwu_ref, awu), (dwd_ref, awd)):
            out[...] = acc[...].astype(BF16)
        plan.at("end")


def ffn_bwd(dh2, o, acts, wo, wg, wu, wd, plan=IDLE, number=None, chunk=512, parts=4):
    tokens, d = dh2.shape
    width, hidden, tile = o.shape[1], wg.shape[1], tokens // parts
    ws = (wo, wg, wu, wd)
    last = len(acts) == 1
    return call(
        functools.partial(_ffn_bwd_kernel, chunk=chunk, last=last), plan, number,
        grid=(tokens // tile,),
        given=[dh2, o, *acts, *ws],
        in_specs=[_rows(tile, d), _rows(tile, width)] + [_rows(tile, a.shape[1]) for a in acts] + [_whole(w.shape) for w in ws],
        out_specs=[_rows(tile, d), _rows(tile, width)] + [_whole(w.shape) for w in ws],
        out_shape=[_like((tokens, d)), _like((tokens, width))] + [_like(w.shape) for w in ws],
        scratch=[pltpu.VMEM(w.shape, F32) for w in ws],
        cost=_cost(4 * tokens * d * (width + 3 * hidden), *acts, dh2, o, *ws, *ws),
    )


def _attend_bwd_kernel(plan, q_ref, k_ref, v_ref, do_ref, o_ref, lse_ref, dq_ref, dk_ref, dv_ref, dq_s, dk_s, dv_s, *, scale, block):
    iq = pl.program_id(0)
    if "start" in plan.schedule:
        pl.when(iq == 0)(lambda: plan.at("start"))
    heads = q_ref.shape[1] // HEAD
    e = scale * LOG2E
    lanes = [slice(i * HEAD, (i + 1) * HEAD) for i in range(heads)]

    @pl.when(iq == 0)
    def _():
        dk_s[...] = jnp.zeros_like(dk_s)
        dv_s[...] = jnp.zeros_like(dv_s)

    dq_s[...] = jnp.zeros_like(dq_s)
    lses = [lse_ref[i : i + 1, :] * LOG2E for i in range(heads)]
    deltas = [(do_ref[:, x].astype(F32) * o_ref[:, x].astype(F32)).T.sum(axis=0, keepdims=True) for x in lanes]

    def part(key, keys, query, queries, masked):
        here, cols = pl.ds(key, keys), slice(query, query + queries)
        scores = [_dot(k_ref[here, x], q_ref[cols, x], 1, 1) for x in lanes]
        dps = [_dot(v_ref[here, x], do_ref[cols, x], 1, 1) for x in lanes]
        ok = _triangle(keys, queries) if masked else None
        for i, x in enumerate(lanes):
            p = jnp.exp2(scores[i] * e - lses[i][:, cols])
            if masked:
                p = jnp.where(ok, p, 0.0)
            ds = (p * (dps[i] - deltas[i][:, cols])).astype(BF16)
            dv_s[here, x] += _dot(p.astype(BF16), do_ref[cols, x], 1, 0)
            dk_s[here, x] += _dot(ds, q_ref[cols, x], 1, 0)
            dq_s[i, :, cols] += _dot(k_ref[here, x].T, ds, 1, 0)

    half = block // 2
    base = pl.multiple_of(iq * block, block)

    def diagonal():
        part(base, half, 0, block, True)
        part(pl.multiple_of(base + half, half), half, half, half, True)

    _blocks(plan, block, lambda key: part(key, block, 0, block, False), diagonal)
    for i, x in enumerate(lanes):
        dq_ref[:, x] = (dq_s[i] * scale).T.astype(BF16)

    @pl.when(iq == pl.num_programs(0) - 1)
    def _():
        dk_ref[...] = (dk_s[...] * scale).astype(BF16)
        dv_ref[...] = dv_s[...].astype(BF16)
        plan.at("end")


def attend_bwd(q, k, v, do, o, lse, plan=IDLE, number=None):
    tokens, width = q.shape
    heads, block = width // HEAD, tokens // 4
    return call(
        functools.partial(_attend_bwd_kernel, scale=HEAD**-0.5, block=block), plan, number,
        grid=(tokens // block,),
        given=[q, k, v, do, o, lse],
        in_specs=[_rows(block, width), _whole(k.shape), _whole(v.shape), _rows(block, width), _rows(block, width),
                  pl.BlockSpec((heads, block), lambda t: (0, t))],
        out_specs=[_rows(block, width), _whole(k.shape), _whole(v.shape)],
        out_shape=[_like((tokens, width))] * 3,
        scratch=[pltpu.VMEM((heads, HEAD, block), F32), pltpu.VMEM(k.shape, F32), pltpu.VMEM(v.shape, F32)],
        cost=_cost(10 * heads * tokens * tokens * HEAD, q, k, v, do, o, q, k, v, exps=heads * tokens * tokens),
    )


def _qkv_bwd_kernel(plan, h_ref, cs_ref, dq_ref, dk_ref, dv_ref, *rest, inner):
    if inner:
        dh1_ref, wq_ref, wk_ref, wv_ref, dh_ref, dwq_ref, dwk_ref, dwv_ref, *accs = rest
    else:
        dwq_ref, dwk_ref, dwv_ref, *accs = rest
    t = pl.program_id(0)
    _point(plan, t, 4)

    @pl.when(t == 0)
    def _():
        for acc in accs:
            acc[...] = jnp.zeros_like(acc)

    wide = h_ref[...].astype(F32)
    scale = _scale(wide)
    a = (wide * scale).astype(BF16)
    c, s = _turns(cs_ref[...])
    grads = [_turn(ref[...].astype(F32), c, -s).astype(BF16) for ref in (dq_ref, dk_ref)] + [dv_ref[...]]
    a_t = a.T
    for acc, g in zip(accs, grads):
        acc[...] += _dot(a_t, g, 1, 0)
    if inner:
        da = sum(_dot(g, w[...], 1, 1) for g, w in zip(grads, (wq_ref, wk_ref, wv_ref)))
        da = da.astype(BF16).astype(F32)
        dh_ref[...] = (dh1_ref[...].astype(F32) + _norm_bwd(wide, scale, da).astype(BF16).astype(F32)).astype(BF16)

    @pl.when(t == pl.num_programs(0) - 1)
    def _():
        for out, acc in zip((dwq_ref, dwk_ref, dwv_ref), accs):
            out[...] = acc[...].astype(BF16)
        plan.at("end")


def qkv_bwd(h, cs, dq, dk, dv, dh1=None, ws=None, plan=IDLE, number=None, parts=4):
    tokens, d = h.shape
    width, tile = dq.shape[1], tokens // parts
    inner = dh1 is not None
    given = [h, cs, dq, dk, dv] + ([dh1, *ws] if inner else [])
    specs = [_rows(tile, d), _rows(tile, HEAD)] + [_rows(tile, width)] * 3 + ([_rows(tile, d)] + [_whole((d, width))] * 3 if inner else [])
    return call(
        functools.partial(_qkv_bwd_kernel, inner=inner), plan, number,
        grid=(tokens // tile,),
        given=given,
        in_specs=specs,
        out_specs=([_rows(tile, d)] if inner else []) + [_whole((d, width))] * 3,
        out_shape=([_like((tokens, d))] if inner else []) + [_like((d, width))] * 3,
        scratch=[pltpu.VMEM((d, width), F32)] * 3,
        cost=_cost((12 if inner else 6) * tokens * d * width, *given),
    )


def adamw(w, m, v, g):
    m = 0.9 * m + 0.1 * g
    v = 0.95 * v + 0.05 * g * g
    step = m * lax.rsqrt(v + 1e-8) + 0.1 * w
    return (w - 0.02 * step).astype(BF16), m, v


def _tail_kernel(plan):
    for point in range(4):
        plan.at(point)


def solution(mesh):
    n = mesh.shape["dp"]

    def flat(w):
        return w.reshape(-1, w.shape[2])

    def step(x, dy, *arrays):
        weights, m, v = (arrays[i : i + 7] for i in (0, 7, 14))
        wq, wk, wv, wo, wg, wu, wd = weights
        layers, width = wq.shape[0], wq.shape[2]
        h = x[0]
        cs = jnp.asarray(_table(h.shape[0]))
        layer = [dict(zip(NAMES, (None,) * 7)) for _ in range(layers)]

        def gathering(names, number, schedule, **more):
            return Gather(n, [(weights[NAMES.index(name)], number) for name in names], schedule, **more)

        def arrived(number, names, got):
            layer[number].update({name: flat(one) for name, one in zip(names, got)})

        def of(number, names):
            return [layer[number][name] for name in names]

        greet = ("greet", ())
        FFN, QKV = ("wo", "wg", "wu", "wd"), ("wq", "wk", "wv")
        kept = []
        for i in range(layers):
            if i == 0:
                names, ws = FFN, None
                plan = Both([gathering(QKV, 0, {}, in_vmem=True), gathering(names, 0, {})],
                            {"start": [(0, *greet), (0, "start", range(3)), (0, "relay", range(3)), (1, "start", (0, 1)), (0, "cross", range(3)),
                                       (0, "finish", range(3))],
                             0: [(1, "relay", (0, 1)), (1, "start", (2,))], 2: [(1, "start", (3,))], 4: [(1, "relay", (2,)), (1, "cross", (0, 1))],
                             7: [(1, "relay", (3,)), (1, "cross", (2,))], "end": [(1, "cross", (3,)), (1, "finish", range(4))]})
            else:
                names, ws = ("wg", "wu"), of(i, QKV)
                plan = gathering(names, i, {"start": [greet, ("start", (0,))], 1: [("start", (1,))], 3: [("relay", (0,))],
                                            5: [("relay", (1,)), ("cross", (0,))], 8: [("cross", (1,))], "end": [("finish", (0, 1))]})
            (q, k, v_, o, lse), got = attend(h, cs, ws, width, plan, 2 + 2 * i)
            arrived(i, names, got)
            if i + 1 < layers:
                names = (*QKV, "wo", "wd")
                plan = gathering(names, i + 1, {(0, 0): [greet, ("start", range(4))], (0, 3): [("start", (4,))], (1, 2): [("relay", range(4))],
                                                (2, 2): [("relay", (4,)), ("cross", range(4))], (3, 1): [("cross", (4,))],
                                                "end": [("finish", range(5))]})
                (h1, h2, g, u), got = ffn(o, h, *of(i, FFN), plan, 3 + 2 * i)
                arrived(i + 1, names, got)
                kept.append((h, q, k, v_, o, lse, (h1, g, u)))
                h = h2
            else:
                kept.append((h, q, k, v_, o, lse, (h,)))
        dh, mine = dy[0], {}

        def scattering(pairs, schedule):
            return Scatter(n, [one for _, one in pairs], schedule)

        def done(pairs, got):
            mine.update({key: one for (key, _), one in zip(pairs, got)})

        waiting = []
        for i in reversed(range(layers)):
            h, q, k, v_, o, lse, acts = kept[i]
            every = range(len(waiting))
            plan = scattering(waiting, {(0, 0): [greet, ("start", every)], (0, 3): [("pair", every)], (1, 3): [("mid", every)],
                                        (3, 1): [("final", every)], "end": [("finish", every)]}) if waiting else IDLE
            (dh1, do, dwo, dwg, dwu, dwd), got = ffn_bwd(dh, o, acts, *of(i, FFN), plan, 20 + 3 * i)
            done(waiting, got)
            rest = [(("wo", i), dwo)]
            now = [(("wg", i), dwg), (("wu", i), dwu), (("wd", i), dwd)]
            if i:
                rest, now = [now[2]] + rest, now[:2]
            more = range(1, len(now))
            points = {"start": [greet, ("start", (0,))], 1: [("pair", (0,)), ("start", more)], 2: [("pair", more)], 3: [("mid", (0,))],
                      5: [("mid", more)], 7: [("final", (0,))], "end": [("final", more), ("finish", range(len(now)))]}
            (dq, dk, dv), got = attend_bwd(q, k, v_, do, o, lse, scattering(now, points), 21 + 3 * i)
            done(now, got)
            if i:
                (dh, *grads), _ = qkv_bwd(h, cs, dq, dk, dv, dh1, of(i, QKV))
            else:
                grads, _ = qkv_bwd(h, cs, dq, dk, dv)
            waiting = rest + [((name, i), one) for name, one in zip(QKV, grads)]
        every = range(len(waiting))
        plan = scattering(waiting, {0: [greet, ("start", every)], 1: [("pair", every)], 2: [("mid", every)],
                                    3: [("final", every), ("finish", every)]})
        _, got = call(_tail_kernel, plan, 18, grid=(), given=[], in_specs=[], out_specs=[], out_shape=[], scratch=[], cost=None)
        done(waiting, got)
        gradients = [jnp.stack([mine[name, i] for i in range(layers)]).astype(F32) for name in NAMES]
        new = [adamw(w.astype(F32), m, v, g) for w, m, v, g in zip(weights, m, v, gradients, strict=True)]
        return tuple(one[which] for which in range(3) for one in new)

    states, cut = P(("rep", "dp"), None, None), P(None, "dp", None)
    return jax.shard_map(
        step,
        mesh=mesh,
        in_specs=(states, states) + (cut,) * 21,
        out_specs=(P("rep", "dp", None),) * 21,
        check_vma=False,
    )
```

```python
import functools

import jax
import jax.numpy as jnp
import numpy as np
from jax import lax
from jax.experimental import pallas as pl
from jax.experimental.pallas import tpu as pltpu
from jax.sharding import PartitionSpec as P

NEG = -1e30
HIDDEN = 2 * NEG
LOG2E = 1.4426950408889634
LN2 = 0.6931471805599453
VMEM = 60 * 2**20
HEAD = 128
THETA = 10000
EPS = 1e-6
NAMES = ("wq", "wk", "wv", "wo", "wg", "wu", "wd")
F32, BF16 = jnp.float32, jnp.bfloat16


NN, NT = ((1,), (0,)), ((1,), (1,))


def _dot(a, b, dims):
    return lax.dot_general(a, b, (dims, ((), ())), preferred_element_type=F32)


def _scale(wide):
    return lax.rsqrt(jnp.mean(wide * wide, -1, keepdims=True) + EPS)


def _norm_bwd(wide, scale, d_normed):
    dot = jnp.sum(d_normed * wide, -1, keepdims=True)
    return d_normed * scale - wide * (dot * scale * scale * scale * (1.0 / wide.shape[-1]))


def _table(tokens):
    half = HEAD // 2
    angle = np.arange(tokens, dtype=np.float64)[:, None] * float(THETA) ** (-np.arange(half, dtype=np.float64) / half)
    return np.concatenate([np.cos(angle), np.sin(angle)], 1).astype(np.float32)


def _turns(cs):
    first = lax.broadcasted_iota(jnp.int32, cs.shape, 1) < HEAD // 2
    other = pltpu.roll(cs, HEAD // 2, 1)
    return jnp.where(first, cs, other), jnp.where(first, -other, cs)


def _turn(t, c, s):
    heads = [t[:, i : i + HEAD] for i in range(0, t.shape[1], HEAD)]
    return jnp.concatenate([x * c + pltpu.roll(x, HEAD // 2, 1) * s for x in heads], 1)


def _whole(shape):
    return pl.BlockSpec(shape, lambda *_: (0,) * len(shape), pipeline_mode=pl.Buffered(1))


def _rows(size, width):
    return pl.BlockSpec((size, width), lambda t: (t, 0))


def _cost(flops, *arrays, exps=0):
    return pl.CostEstimate(flops=int(flops), transcendentals=int(exps), bytes_accessed=int(sum(a.size * a.dtype.itemsize for a in arrays)))


def _params(**more):
    return pltpu.CompilerParams(vmem_limit_bytes=VMEM, **more)


def _like(shape, dtype=BF16):
    return jax.ShapeDtypeStruct(shape, dtype)


MESH = pl.DeviceIdType.MESH
ANY = pl.BlockSpec(memory_space=pl.ANY)
SLOTS = 9


class _Place:
    def __init__(self, n):
        me = lax.axis_index("dp")
        self.me, self.core, self.chip = me, lax.rem(me, 2), lax.div(me, 2)
        chips = n // 2
        self.chips = chips
        self.right_chip = lax.rem(self.chip + 1, chips)
        self.left_chip = lax.rem(self.chip + chips - 1, chips)
        self.across_chip = lax.rem(self.chip + 2, chips)
        self.right, self.left, self.across = (c * 2 + self.core for c in (self.right_chip, self.left_chip, self.across_chip))
        self.partner = self.chip * 2 + 1 - self.core

    def greet(self):
        barrier = pltpu.get_barrier_semaphore()
        for peer in (self.right, self.left, self.partner):
            pl.semaphore_signal(barrier, inc=1, device_id={"dp": peer}, device_id_type=MESH)
        pl.semaphore_wait(barrier, 3)


def _halves(rows):
    return pl.ds(0, rows // 2), pl.ds(rows // 2, rows // 2)


class Gather:
    def __init__(self, n, given, schedule, in_vmem=False):
        self.n, self.given, self.schedule = n, given, schedule
        self.inputs = [a for a, _ in given]
        shapes = [(n, *a.shape[1:]) for a, _ in given]
        self.out_shape = [] if in_vmem else [_like(s) for s in shapes]
        self.scratch = [pltpu.SemaphoreType.DMA((len(given), SLOTS))] * 2 + [pltpu.VMEM(s if in_vmem else s[1:], BF16) for s in shapes]

    def bind(self, ins, outs, scratch):
        self.send, self.recv = scratch[:2]
        self.src = [ref.at[layer] for ref, (_, layer) in zip(ins, self.given)]
        self.dst, self.own = (outs, scratch[2:]) if outs else (scratch[2:], None)
        self.place = _Place(self.n)
        return self

    def _copy(self, i, slot):
        p, src, dst = self.place, self.src[i], self.dst[i]
        first, second = _halves(src.shape[0])
        sends = {
            0: (src, dst.at[p.me], p.right),
            1: (src, dst.at[p.me], p.left),
            2: (src, dst.at[p.me], p.partner),
            3: (dst.at[p.left, first], dst.at[p.left, first], p.right),
            4: (dst.at[p.right, second], dst.at[p.right, second], p.left),
            5: (dst.at[p.left], dst.at[p.left], p.partner),
            6: (dst.at[p.right], dst.at[p.right], p.partner),
            7: (dst.at[p.across], dst.at[p.across], p.partner),
        }
        if slot == 8:
            return pltpu.make_async_copy(src, self.own[i] if self.own else dst.at[p.me], self.send.at[i, 8])
        if slot == 9:
            return pltpu.make_async_copy(self.own[i], dst.at[p.me], self.recv.at[i, 8])
        a, b, to = sends[slot]
        return pltpu.make_async_remote_copy(a, b, self.send.at[i, slot], self.recv.at[i, slot], device_id={"dp": to}, device_id_type=MESH)

    def start(self, i):
        for slot in (0, 1, 2, 8):
            self._copy(i, slot).start()

    def relay(self, i):
        for arrived, on in ((0, (3, 5)), (1, (4, 6))):
            self._copy(i, arrived).wait_recv()
            for slot in on:
                self._copy(i, slot).start()
        if self.own:
            self._copy(i, 8).wait()
            self._copy(i, 9).start()

    def cross(self, i):
        self._copy(i, 3).wait_recv()
        self._copy(i, 4).wait_recv()
        self._copy(i, 7).start()

    def finish(self, i):
        for slot in (2, 5, 6, 7):
            self._copy(i, slot).wait_recv()
        for slot in range(8):
            self._copy(i, slot).wait_send()
        self._copy(i, 9 if self.own else 8).wait()

    def at(self, point):
        _run(self, point)


class Scatter:
    def __init__(self, n, grads, schedule):
        self.n, self.schedule = n, schedule
        chips = n // 2
        blocks = [(g.shape[0] // n, g.shape[1]) for g in grads]
        self.count = len(grads)
        self.inputs = [g.reshape(chips, 2, *b) for g, b in zip(grads, blocks)]
        self.out_shape = [_like(b) for b in blocks]
        self.scratch = [pltpu.SemaphoreType.DMA((self.count, SLOTS))] * 2
        for r, c in blocks:
            self.scratch += [pltpu.VMEM((chips, r, c), BF16)] * 2 + [pltpu.VMEM((r, c), BF16)] * 2 + [pltpu.VMEM((r // 2, c), BF16)] * 2

    def bind(self, ins, outs, scratch):
        self.send, self.recv = scratch[:2]
        self.ins, self.outs = ins, outs
        self.bufs = [scratch[2 + 6 * i : 8 + 6 * i] for i in range(self.count)]
        self.place = _Place(self.n)
        return self

    def _copy(self, i, slot):
        p = self.place
        own, got, from_left, from_right, mid_left, mid_right = self.bufs[i]
        first, second = _halves(from_left.shape[0])
        if slot == 7:
            return pltpu.make_async_copy(from_left, self.outs[i], self.send.at[i, 7])
        if slot == 8:
            return pltpu.make_async_copy(self.ins[i].at[:, p.core], own, self.send.at[i, 8])
        a, b, to = {
            0: (self.ins[i].at[:, 1 - p.core], got, p.partner),
            1: (own.at[p.across_chip, first], mid_left, p.right),
            2: (own.at[p.across_chip, second], mid_right, p.left),
            3: (own.at[p.right_chip, second], from_left.at[second], p.right),
            4: (own.at[p.left_chip, first], from_right.at[first], p.left),
            5: (own.at[p.right_chip, first], from_left.at[first], p.right),
            6: (own.at[p.left_chip, second], from_right.at[second], p.left),
        }[slot]
        return pltpu.make_async_remote_copy(a, b, self.send.at[i, slot], self.recv.at[i, slot], device_id={"dp": to}, device_id_type=MESH)

    def start(self, i):
        self._copy(i, 0).start()
        self._copy(i, 8).start()

    def pair(self, i):
        own, got = self.bufs[i][:2]
        self._copy(i, 8).wait()
        self._copy(i, 0).wait_recv()

        def add(j, _):
            own[j] = (own[j].astype(F32) + got[j].astype(F32)).astype(BF16)

        lax.fori_loop(0, self.place.chips, add, None)
        self._copy(i, 1).start()
        self._copy(i, 2).start()

    def mid(self, i):
        p = self.place
        own, _, _, _, mid_left, mid_right = self.bufs[i]
        first, second = _halves(own.shape[1])
        for slot, chip, half, arrived in ((1, p.right_chip, first, mid_left), (2, p.left_chip, second, mid_right)):
            self._copy(i, slot).wait_recv()
            own[chip, half] = (own[chip, half].astype(F32) + arrived[...].astype(F32)).astype(BF16)
        for slot in (5, 6, 3, 4):
            self._copy(i, slot).start()

    def final(self, i):
        own, _, from_left, from_right, _, _ = self.bufs[i]
        for slot in (3, 4, 5, 6):
            self._copy(i, slot).wait_recv()
        total = own[self.place.chip].astype(F32) + from_left[...].astype(F32) + from_right[...].astype(F32)
        from_left[...] = total.astype(BF16)
        self._copy(i, 7).start()

    def finish(self, i):
        for slot in range(7):
            self._copy(i, slot).wait_send()
        self._copy(i, 7).wait()

    def at(self, point):
        _run(self, point)


def _run(plan, point):
    for name, items in plan.schedule.get(point, ()):
        _act(plan, name, items)


def _act(plan, name, items):
    if name == "greet":
        plan.place.greet()
    for i in items:
        getattr(plan, name)(i)


def _point(plan, t, steps, *rest):
    for step in range(steps):
        key = (step, *rest) if rest else step
        if key in plan.schedule:
            pl.when(t == step)(functools.partial(plan.at, key))


class _Idle:
    inputs, out_shape, scratch, schedule = [], [], [], {}

    def bind(self, *_):
        return self

    def at(self, point):
        pass


IDLE = _Idle()


def call(kernel, plan, number, *, grid, given, in_specs, out_specs, out_shape, scratch, cost):
    sizes = [len(given), len(plan.inputs), len(out_shape), len(plan.out_shape), len(scratch), len(plan.scratch)]
    ends = [sum(sizes[:i]) for i in range(7)]

    def body(*refs):
        a, b, c, d, e, f = (refs[ends[i] : ends[i + 1]] for i in range(6))
        kernel(plan.bind(b, d, f), *a, *c, *e)

    more = dict(collective_id=number, has_side_effects=True) if plan.inputs else {}
    got = pl.pallas_call(
        body,
        grid=grid,
        in_specs=in_specs + [ANY] * sizes[1],
        out_specs=out_specs + [ANY] * sizes[3],
        out_shape=out_shape + plan.out_shape,
        scratch_shapes=scratch + plan.scratch,
        compiler_params=_params(**more),
        cost_estimate=cost,
    )(*given, *plan.inputs)
    return got[: sizes[2]], got[sizes[2] :]


def adamw(w, m, v, g):
    m = 0.9 * m + 0.1 * g
    v = 0.95 * v + 0.05 * g * g
    step = m * lax.rsqrt(v + 1e-8) + 0.1 * w
    return (w - 0.02 * step).astype(BF16), m, v


class Both:
    def __init__(self, plans, schedule):
        self.plans, self.schedule = plans, schedule
        self.inputs, self.out_shape, self.scratch = (sum((getattr(p, x) for p in plans), []) for x in ("inputs", "out_shape", "scratch"))

    def bind(self, ins, outs, scratch):
        for p in self.plans:
            a, b, c = len(p.inputs), len(p.out_shape), len(p.scratch)
            p.bind(ins[:a], outs[:b], scratch[:c])
            ins, outs, scratch = ins[a:], outs[b:], scratch[c:]
        return self

    def at(self, point):
        for number, name, items in self.schedule.get(point, ()):
            _act(self.plans[number], name, items)


def _blocks(plan, block, causal_part, diagonal):
    iq, steps = pl.program_id(0), 4
    named = {i * (i + 1) // 2 + j: (i, j) for i in range(steps) for j in range(i + 1)}

    def ahead(inside, j=None):
        for number, (i, at) in named.items():
            if number in plan.schedule and (at < i) == inside:
                pl.when((iq == i) & (j == at) if inside else iq == i)(functools.partial(plan.at, number))

    def loop(j, _):
        ahead(True, j)
        causal_part(pl.multiple_of(j * block, block))

    lax.fori_loop(0, iq, loop, None)
    ahead(False)
    diagonal()


def _triangle(keys, queries):
    return lax.broadcasted_iota(jnp.int32, (keys, queries), 1) >= lax.broadcasted_iota(jnp.int32, (keys, queries), 0)


def _attend_kernel(plan, h_ref, cs_ref, *rest, scale, block, early):
    iq = pl.program_id(0)
    if "start" in plan.schedule:
        pl.when(iq == 0)(lambda: plan.at("start"))
    if early:
        wq_ref, wk_ref, wv_ref = (ref.reshape(-1, ref.shape[2]) for ref in plan.plans[0].dst)
    else:
        wq_ref, wk_ref, wv_ref, *rest = rest
    q_ref, k_out, v_out, o_ref, lse_ref, k_ref, v_ref, top_s, mix_s = rest
    here = pl.ds(pl.multiple_of(iq * block, block), block)
    wide = h_ref[...].astype(F32)
    a = (wide * _scale(wide)).astype(BF16)
    c, s = _turns(cs_ref[...])
    v = _dot(a, wv_ref[...], NN).astype(BF16)
    v_out[...] = v
    v_ref[here, :] = v
    q_ref[...] = _turn(_dot(a, wq_ref[...], NN).astype(BF16).astype(F32), c, s).astype(BF16)
    k = _turn(_dot(a, wk_ref[...], NN).astype(BF16).astype(F32), c, s).astype(BF16)
    k_out[...] = k
    k_ref[here, :] = k
    heads = q_ref.shape[1] // HEAD
    e = scale * LOG2E
    lanes = [slice(i * HEAD, (i + 1) * HEAD) for i in range(heads)]
    top_s[...] = jnp.full(top_s.shape, NEG, F32)
    mix_s[...] = jnp.zeros_like(mix_s)

    def part(key, keys, query, queries, masked):
        here, cols = pl.ds(key, keys), slice(query, query + queries)
        scores = [_dot(k_ref[here, x], q_ref[cols, x], NT) for x in lanes]
        ok = _triangle(keys, queries) if masked else None
        ones = jnp.ones((8, keys), BF16)
        weights, keeps = [], []
        for i, s in enumerate(scores):
            if masked:
                s = jnp.where(ok, s, HIDDEN)
            old = top_s[i : i + 1, cols]
            top = jnp.maximum(old, s.max(axis=0, keepdims=True))
            top_s[i : i + 1, cols] = top
            weights.append(jnp.exp2((s - top) * e).astype(BF16))
            keeps.append(jnp.exp2((old - top) * e))
        for i, (p, keep) in enumerate(zip(weights, keeps)):
            values = jnp.concatenate([v_ref[here, lanes[i]].T, ones], axis=0)
            mix_s[i, :, cols] = mix_s[i, :, cols] * keep + _dot(values, p, NN)

    half = block // 2
    base = pl.multiple_of(iq * block, block)

    def diagonal():
        part(base, half, 0, block, True)
        part(pl.multiple_of(base + half, half), half, half, half, True)

    _blocks(plan, block, lambda key: part(key, block, 0, block, False), diagonal)
    for i, x in enumerate(lanes):
        total = mix_s[i, HEAD : HEAD + 1, :]
        o_ref[:, x] = (mix_s[i, :HEAD, :] * (1 / total)).T.astype(BF16)
        lse_ref[i : i + 1, :] = top_s[i : i + 1, :] * scale + jnp.log(total)
    if "end" in plan.schedule:
        pl.when(iq == pl.num_programs(0) - 1)(lambda: plan.at("end"))


def attend(h, cs, ws, width, plan=IDLE, number=0):
    tokens, d = h.shape
    heads, block = width // HEAD, tokens // 4
    early = ws is None
    return call(
        functools.partial(_attend_kernel, scale=HEAD**-0.5, block=block, early=early), plan, number,
        grid=(tokens // block,),
        given=[h, cs] + list(ws or ()),
        in_specs=[_rows(block, d), _rows(block, HEAD)] + [_whole((d, width))] * (0 if early else 3),
        out_specs=[_rows(block, width)] * 4 + [pl.BlockSpec((heads, block), lambda t: (0, t))],
        out_shape=[_like((tokens, width))] * 4 + [_like((heads, tokens), F32)],
        scratch=[pltpu.VMEM((tokens, width), BF16)] * 2 + [pltpu.VMEM((heads, block), F32), pltpu.VMEM((heads, HEAD + 8, block), F32)],
        cost=_cost(4 * heads * tokens * tokens * HEAD + 6 * tokens * d * width, h, h, h, h, h, exps=heads * tokens * tokens),
    )


def _ffn_kernel(plan, o_ref, h_ref, wo_ref, wg_ref, wu_ref, wd_ref, h1_ref, h2_ref, g_ref, u_ref, *, chunk):
    t = pl.program_id(0)
    _point(plan, t, 4, 0)
    h1 = (h_ref[...].astype(F32) + _dot(o_ref[...], wo_ref[...], NN).astype(BF16).astype(F32)).astype(BF16)
    h1_ref[...] = h1
    wide = h1.astype(F32)
    b = (wide * _scale(wide)).astype(BF16)
    total = None
    for at in range(0, wg_ref.shape[1], chunk):
        here = slice(at, at + chunk)
        if at:
            _point(plan, t, 4, at // chunk)
        gate, up = _dot(b, wg_ref[:, here], NN), _dot(b, wu_ref[:, here], NN)
        g_ref[:, here] = gate
        u_ref[:, here] = up
        act = (gate * jax.nn.sigmoid(gate) * up).astype(BF16)
        term = _dot(act, wd_ref[here, :], NN)
        total = term if total is None else total + term
    h2_ref[...] = (wide + total.astype(BF16).astype(F32)).astype(BF16)
    if "end" in plan.schedule:
        pl.when(t == pl.num_programs(0) - 1)(lambda: plan.at("end"))


def ffn(o, h, wo, wg, wu, wd, plan=IDLE, number=0, chunk=512, parts=4):
    tokens, d = h.shape
    width, hidden, tile = o.shape[1], wg.shape[1], tokens // parts
    return call(
        functools.partial(_ffn_kernel, chunk=chunk), plan, number,
        grid=(tokens // tile,),
        given=[o, h, wo, wg, wu, wd],
        in_specs=[_rows(tile, width), _rows(tile, d)] + [_whole(w.shape) for w in (wo, wg, wu, wd)],
        out_specs=[_rows(tile, d)] * 2 + [_rows(tile, hidden)] * 2,
        out_shape=[_like((tokens, d))] * 2 + [_like((tokens, hidden), F32)] * 2,
        scratch=[],
        cost=_cost(2 * tokens * d * (width + 3 * hidden), o, h, h, h, wo, wg, wu, wd),
    )


def _ffn_bwd_kernel(plan, dh2_ref, o_ref, *rest, chunk, last):
    if last:
        h_ref, *rest = rest
    else:
        h1_ref, g_ref, u_ref, *rest = rest
    wo_ref, wg_ref, wu_ref, wd_ref, dh1_ref, do_ref, dwo_ref, dwg_ref, dwu_ref, dwd_ref, awo, awg, awu, awd = rest
    t = pl.program_id(0)
    _point(plan, t, 4, 0)

    @pl.when(t == 0)
    def _():
        for acc in (awo, awg, awu, awd):
            acc[...] = jnp.zeros_like(acc)

    dh2, o = dh2_ref[...], o_ref[...]
    if last:
        wide = (h_ref[...].astype(F32) + _dot(o, wo_ref[...], NN).astype(BF16).astype(F32)).astype(BF16).astype(F32)
    else:
        wide = h1_ref[...].astype(F32)
    scale = _scale(wide)
    b = (wide * scale).astype(BF16)
    b_t = b.T
    db = None
    for at in range(0, wg_ref.shape[1], chunk):
        here = slice(at, at + chunk)
        if at:
            _point(plan, t, 4, at // chunk)
        d_act = _dot(dh2, wd_ref[here, :], NT).astype(BF16).astype(F32)
        if last:
            gate, up = _dot(b, wg_ref[:, here], NN), _dot(b, wu_ref[:, here], NN)
        else:
            gate, up = g_ref[:, here], u_ref[:, here]
        sig = jax.nn.sigmoid(gate)
        silu = gate * sig
        act = (silu * up).astype(BF16)
        d_up = (d_act * silu).astype(BF16)
        d_gate = (d_act * up * (sig + silu * (1 - sig))).astype(BF16)
        term = _dot(d_gate, wg_ref[:, here], NT) + _dot(d_up, wu_ref[:, here], NT)
        db = term if db is None else db + term
        awd[here, :] += _dot(act.T, dh2, NN)
        awg[:, here] += _dot(b_t, d_gate, NN)
        awu[:, here] += _dot(b_t, d_up, NN)
    db = db.astype(BF16).astype(F32)
    dh1 = (dh2.astype(F32) + _norm_bwd(wide, scale, db).astype(BF16).astype(F32)).astype(BF16)
    dh1_ref[...] = dh1
    do_ref[...] = _dot(dh1, wo_ref[...], NT).astype(BF16)
    awo[...] += _dot(o.T, dh1, NN)

    @pl.when(t == pl.num_programs(0) - 1)
    def _():
        for out, acc in ((dwo_ref, awo), (dwg_ref, awg), (dwu_ref, awu), (dwd_ref, awd)):
            out[...] = acc[...].astype(BF16)
        plan.at("end")


def ffn_bwd(dh2, o, acts, wo, wg, wu, wd, plan=IDLE, number=0, chunk=512, parts=4):
    tokens, d = dh2.shape
    width, hidden, tile = o.shape[1], wg.shape[1], tokens // parts
    ws = (wo, wg, wu, wd)
    last = len(acts) == 1
    return call(
        functools.partial(_ffn_bwd_kernel, chunk=chunk, last=last), plan, number,
        grid=(tokens // tile,),
        given=[dh2, o, *acts, *ws],
        in_specs=[_rows(tile, d), _rows(tile, width)] + [_rows(tile, a.shape[1]) for a in acts] + [_whole(w.shape) for w in ws],
        out_specs=[_rows(tile, d), _rows(tile, width)] + [_whole(w.shape) for w in ws],
        out_shape=[_like((tokens, d)), _like((tokens, width))] + [_like(w.shape) for w in ws],
        scratch=[pltpu.VMEM(w.shape, F32) for w in ws],
        cost=_cost(4 * tokens * d * (width + 3 * hidden), *acts, dh2, o, *ws, *ws),
    )


def _attend_bwd_kernel(plan, q_ref, k_ref, v_ref, do_ref, o_ref, lse_ref, dq_ref, dk_ref, dv_ref, dq_s, dk_s, dv_s, *, scale, block):
    iq = pl.program_id(0)
    if "start" in plan.schedule:
        pl.when(iq == 0)(lambda: plan.at("start"))
    heads = q_ref.shape[1] // HEAD
    e = scale * LOG2E
    lanes = [slice(i * HEAD, (i + 1) * HEAD) for i in range(heads)]

    @pl.when(iq == 0)
    def _():
        dk_s[...] = jnp.zeros_like(dk_s)
        dv_s[...] = jnp.zeros_like(dv_s)

    dq_s[...] = jnp.zeros_like(dq_s)
    lses = [lse_ref[i : i + 1, :] * LOG2E for i in range(heads)]
    deltas = [(do_ref[:, x].astype(F32) * o_ref[:, x].astype(F32)).T.sum(axis=0, keepdims=True) for x in lanes]

    def part(key, keys, query, queries, masked):
        here, cols = pl.ds(key, keys), slice(query, query + queries)
        scores = [_dot(k_ref[here, x], q_ref[cols, x], NT) for x in lanes]
        dps = [_dot(v_ref[here, x], do_ref[cols, x], NT) for x in lanes]
        ok = _triangle(keys, queries) if masked else None
        for i, x in enumerate(lanes):
            p = jnp.exp2(scores[i] * e - lses[i][:, cols])
            if masked:
                p = jnp.where(ok, p, 0.0)
            ds = (p * (dps[i] - deltas[i][:, cols])).astype(BF16)
            dv_s[here, x] += _dot(p.astype(BF16), do_ref[cols, x], NN)
            dk_s[here, x] += _dot(ds, q_ref[cols, x], NN)
            dq_s[i, :, cols] += _dot(k_ref[here, x].T, ds, NN)

    half = block // 2
    base = pl.multiple_of(iq * block, block)

    def diagonal():
        part(base, half, 0, block, True)
        part(pl.multiple_of(base + half, half), half, half, half, True)

    _blocks(plan, block, lambda key: part(key, block, 0, block, False), diagonal)
    for i, x in enumerate(lanes):
        dq_ref[:, x] = (dq_s[i] * scale).T.astype(BF16)

    @pl.when(iq == pl.num_programs(0) - 1)
    def _():
        dk_ref[...] = (dk_s[...] * scale).astype(BF16)
        dv_ref[...] = dv_s[...].astype(BF16)
        plan.at("end")


def attend_bwd(q, k, v, do, o, lse, plan=IDLE, number=0):
    tokens, width = q.shape
    heads, block = width // HEAD, tokens // 4
    return call(
        functools.partial(_attend_bwd_kernel, scale=HEAD**-0.5, block=block), plan, number,
        grid=(tokens // block,),
        given=[q, k, v, do, o, lse],
        in_specs=[_rows(block, width), _whole(k.shape), _whole(v.shape), _rows(block, width), _rows(block, width),
                  pl.BlockSpec((heads, block), lambda t: (0, t))],
        out_specs=[_rows(block, width), _whole(k.shape), _whole(v.shape)],
        out_shape=[_like((tokens, width))] * 3,
        scratch=[pltpu.VMEM((heads, HEAD, block), F32), pltpu.VMEM(k.shape, F32), pltpu.VMEM(v.shape, F32)],
        cost=_cost(10 * heads * tokens * tokens * HEAD, q, k, v, do, o, q, k, v, exps=heads * tokens * tokens),
    )


def _qkv_bwd_kernel(plan, h_ref, cs_ref, dq_ref, dk_ref, dv_ref, *rest, inner, updates):
    layers = rest[0].shape[0] if updates else 0
    per = 3 + layers
    states, rest = rest[: per * updates], rest[per * updates :]
    results, rest = rest[3 : 3 + 3 * updates], rest[:3] + rest[3 + 3 * updates :]
    for i in range(updates):
        w_ref, m_ref, v_ref, *gs = states[per * i : per * i + per]
        for at, g_ref in enumerate(gs):
            new = adamw(w_ref[at].astype(F32), m_ref[at], v_ref[at], g_ref[...].astype(F32))
            for out, one in zip(results[3 * i : 3 * i + 3], new):
                out[at] = one
    if inner:
        dh1_ref, wq_ref, wk_ref, wv_ref, dh_ref, dwq_ref, dwk_ref, dwv_ref, *accs = rest
    else:
        dwq_ref, dwk_ref, dwv_ref, *accs = rest
    t = pl.program_id(0)
    _point(plan, t, 4)

    @pl.when(t == 0)
    def _():
        for acc in accs:
            acc[...] = jnp.zeros_like(acc)

    wide = h_ref[...].astype(F32)
    scale = _scale(wide)
    a = (wide * scale).astype(BF16)
    c, s = _turns(cs_ref[...])
    grads = [_turn(ref[...].astype(F32), c, -s).astype(BF16) for ref in (dq_ref, dk_ref)] + [dv_ref[...]]
    a_t = a.T
    for acc, g in zip(accs, grads):
        acc[...] += _dot(a_t, g, NN)
    if inner:
        da = sum(_dot(g, w[...], NT) for g, w in zip(grads, (wq_ref, wk_ref, wv_ref)))
        da = da.astype(BF16).astype(F32)
        dh_ref[...] = (dh1_ref[...].astype(F32) + _norm_bwd(wide, scale, da).astype(BF16).astype(F32)).astype(BF16)

    @pl.when(t == pl.num_programs(0) - 1)
    def _():
        for out, acc in zip((dwq_ref, dwk_ref, dwv_ref), accs):
            out[...] = acc[...].astype(BF16)
        plan.at("end")


def qkv_bwd(h, cs, dq, dk, dv, dh1=None, ws=None, updates=(), plan=IDLE, number=0, parts=4):
    tokens, d = h.shape
    width, tile = dq.shape[1], tokens // parts
    inner = dh1 is not None
    given = [h, cs, dq, dk, dv] + ([dh1, *ws] if inner else [])
    specs = [_rows(tile, d), _rows(tile, HEAD)] + [_rows(tile, width)] * 3 + ([_rows(tile, d)] + [_whole((d, width))] * 3 if inner else [])
    outs, shapes = [], []
    for w, m, v, *gs in updates:
        layers, rows, columns = w.shape
        cut = pl.BlockSpec((layers, rows // parts, columns), lambda t: (0, t, 0))
        given += [w, m, v, *gs]
        specs += [cut] * 3 + [_rows(rows // parts, columns)] * layers
        outs += [cut] * 3
        shapes += [_like(w.shape), _like(w.shape, F32), _like(w.shape, F32)]
    return call(
        functools.partial(_qkv_bwd_kernel, inner=inner, updates=len(updates)), plan, number,
        grid=(tokens // tile,),
        given=given,
        in_specs=specs,
        out_specs=([_rows(tile, d)] if inner else []) + [_whole((d, width))] * 3 + outs,
        out_shape=([_like((tokens, d))] if inner else []) + [_like((d, width))] * 3 + shapes,
        scratch=[pltpu.VMEM((d, width), F32)] * 3,
        cost=_cost((12 if inner else 6) * tokens * d * width, *given),
    )


def _tail_kernel(plan):
    for point in range(4):
        plan.at(point)


def solution(mesh):
    n = mesh.shape["dp"]

    def flat(w):
        return w.reshape(-1, w.shape[2])

    def step(x, dy, *arrays):
        weights, m, v = (arrays[i : i + 7] for i in (0, 7, 14))
        wq, wk, wv, wo, wg, wu, wd = weights
        layers, width = wq.shape[0], wq.shape[2]
        h = x[0]
        cs = jnp.asarray(_table(h.shape[0]))
        layer = [dict(zip(NAMES, (None,) * 7)) for _ in range(layers)]

        def gathering(names, number, schedule, **more):
            return Gather(n, [(weights[NAMES.index(name)], number) for name in names], schedule, **more)

        def arrived(number, names, got):
            layer[number].update({name: flat(one) for name, one in zip(names, got)})

        def of(number, names):
            return [layer[number][name] for name in names]

        greet = ("greet", ())
        FFN, QKV = ("wo", "wg", "wu", "wd"), ("wq", "wk", "wv")
        kept = []
        for i in range(layers):
            if i == 0:
                names, ws = FFN, None
                plan = Both([gathering(QKV, 0, {}, in_vmem=True), gathering(names, 0, {})],
                            {"start": [(0, *greet), (0, "start", range(3)), (0, "relay", range(3)), (1, "start", (0, 1)), (0, "cross", range(3)),
                                       (1, "start", (2, 3)), (0, "finish", range(3))],
                             2: [(1, "relay", (0, 1))], 5: [(1, "relay", (2, 3))], 8: [(1, "cross", (0, 1))],
                             "end": [(1, "cross", (2, 3)), (1, "finish", range(4))]})
            else:
                names, ws = ("wg", "wu"), of(i, QKV)
                plan = gathering(names, i, {"start": [greet, ("start", (0, 1))], 5: [("relay", (0, 1))], 9: [("cross", (0,))],
                                            "end": [("cross", (1,)), ("finish", (0, 1))]})
            (q, k, v_, o, lse), got = attend(h, cs, ws, width, plan, 2 + 2 * i)
            arrived(i, names, got)
            if i + 1 < layers:
                names = (*QKV, "wo", "wd")
                plan = gathering(names, i + 1, {(0, 0): [greet, ("start", range(5))], (2, 2): [("relay", range(5))], (3, 3): [("cross", range(4))],
                                                "end": [("cross", (4,)), ("finish", range(5))]})
                (h1, h2, g, u), got = ffn(o, h, *of(i, FFN), plan, 3 + 2 * i)
                arrived(i + 1, names, got)
                kept.append((h, q, k, v_, o, lse, (h1, g, u)))
                h = h2
            else:
                kept.append((h, q, k, v_, o, lse, (h,)))
        dh, mine = dy[0], {}

        def scattering(pairs, schedule):
            return Scatter(n, [one for _, one in pairs], schedule)

        def done(pairs, got):
            mine.update({key: one for (key, _), one in zip(pairs, got)})

        waiting = []
        for i in reversed(range(layers)):
            h, q, k, v_, o, lse, acts = kept[i]
            every = range(len(waiting))
            plan = scattering(waiting, {(0, 0): [greet, ("start", every)], (1, 0): [("pair", every)], (2, 0): [("mid", every)],
                                        "end": [("final", every), ("finish", every)]}) if waiting else IDLE
            (dh1, do, dwo, dwg, dwu, dwd), got = ffn_bwd(dh, o, acts, *of(i, FFN), plan, 20 + 3 * i)
            done(waiting, got)
            rest = [(("wo", i), dwo)]
            now = [(("wg", i), dwg), (("wu", i), dwu), (("wd", i), dwd)]
            if i:
                rest, now = [now[2]] + rest, now[:2]
            more = range(1, len(now))
            points = {"start": [greet, ("start", (0,))], 1: [("pair", (0,)), ("start", more)], 2: [("pair", more)], 3: [("mid", (0,))],
                      5: [("mid", more)], 7: [("final", (0,))], "end": [("final", more), ("finish", range(len(now)))]}
            (dq, dk, dv), got = attend_bwd(q, k, v_, do, o, lse, scattering(now, points), 21 + 3 * i)
            done(now, got)
            if i:
                (dh, *grads), _ = qkv_bwd(h, cs, dq, dk, dv, dh1, of(i, QKV))
            else:
                updates = [(weights[k], m[k], v[k], *(mine[NAMES[k], j] for j in range(layers))) for k in (4, 5, 6)]
                (*grads, a, b, c, d, e, f, x_, y_, z_), _ = qkv_bwd(h, cs, dq, dk, dv, updates=updates)
                ffn_new = [(a, b, c), (d, e, f), (x_, y_, z_)]
            waiting = rest + [((name, i), one) for name, one in zip(QKV, grads)]
        every = range(len(waiting))
        plan = scattering(waiting, {0: [greet, ("start", every)], 1: [("pair", every)], 2: [("mid", every)],
                                    3: [("final", every), ("finish", every)]})
        _, got = call(_tail_kernel, plan, 18, grid=(), given=[], in_specs=[], out_specs=[], out_shape=[], scratch=[], cost=None)
        done(waiting, got)
        gradients = [jnp.stack([mine[name, i] for i in range(layers)]).astype(F32) for name in NAMES[:4]]
        new = [adamw(w.astype(F32), m, v, g) for w, m, v, g in zip(weights[:4], m[:4], v[:4], gradients, strict=True)] + ffn_new
        return tuple(one[which] for which in range(3) for one in new)

    states, cut = P(("rep", "dp"), None, None), P(None, "dp", None)
    return jax.shard_map(
        step,
        mesh=mesh,
        in_specs=(states, states) + (cut,) * 21,
        out_specs=(P("rep", "dp", None),) * 21,
        check_vma=False,
    )
```

```python
import functools

import jax
import jax.numpy as jnp
import numpy as np
from jax import lax
from jax.experimental import pallas as pl
from jax.experimental.pallas import tpu as pltpu
from jax.sharding import PartitionSpec as P

NEG = -1e30
HIDDEN = 2 * NEG
LOG2E = 1.4426950408889634
LN2 = 0.6931471805599453
VMEM = 60 * 2**20
HEAD = 128
THETA = 10000
EPS = 1e-6
NAMES = ("wq", "wk", "wv", "wo", "wg", "wu", "wd")
F32, BF16 = jnp.float32, jnp.bfloat16


NN, NT = ((1,), (0,)), ((1,), (1,))


def _dot(a, b, dims):
    return lax.dot_general(a, b, (dims, ((), ())), preferred_element_type=F32)


def _scale(wide):
    return lax.rsqrt(jnp.mean(wide * wide, -1, keepdims=True) + EPS)


def _norm_bwd(wide, scale, d_normed):
    dot = jnp.sum(d_normed * wide, -1, keepdims=True)
    return d_normed * scale - wide * (dot * scale * scale * scale * (1.0 / wide.shape[-1]))


def _table(tokens):
    half = HEAD // 2
    angle = np.arange(tokens, dtype=np.float64)[:, None] * float(THETA) ** (-np.arange(half, dtype=np.float64) / half)
    return np.concatenate([np.cos(angle), np.sin(angle)], 1).astype(np.float32)


def _turns(cs):
    first = lax.broadcasted_iota(jnp.int32, cs.shape, 1) < HEAD // 2
    other = pltpu.roll(cs, HEAD // 2, 1)
    return jnp.where(first, cs, other), jnp.where(first, -other, cs)


def _turn(t, c, s):
    heads = [t[:, i : i + HEAD] for i in range(0, t.shape[1], HEAD)]
    return jnp.concatenate([x * c + pltpu.roll(x, HEAD // 2, 1) * s for x in heads], 1)


def _whole(shape):
    return pl.BlockSpec(shape, lambda *_: (0,) * len(shape), pipeline_mode=pl.Buffered(1))


def _rows(size, width):
    return pl.BlockSpec((size, width), lambda t: (t, 0))


def _cost(flops, *arrays, exps=0):
    return pl.CostEstimate(flops=int(flops), transcendentals=int(exps), bytes_accessed=int(sum(a.size * a.dtype.itemsize for a in arrays)))


def _params(**more):
    return pltpu.CompilerParams(vmem_limit_bytes=VMEM, **more)


def _like(shape, dtype=BF16):
    return jax.ShapeDtypeStruct(shape, dtype)


MESH = pl.DeviceIdType.MESH
ANY = pl.BlockSpec(memory_space=pl.ANY)
SLOTS = 9


class _Place:
    def __init__(self, n):
        me = lax.axis_index("dp")
        self.me, self.core, self.chip = me, lax.rem(me, 2), lax.div(me, 2)
        chips = n // 2
        self.chips = chips
        self.right_chip = lax.rem(self.chip + 1, chips)
        self.left_chip = lax.rem(self.chip + chips - 1, chips)
        self.across_chip = lax.rem(self.chip + 2, chips)
        self.right, self.left, self.across = (c * 2 + self.core for c in (self.right_chip, self.left_chip, self.across_chip))
        self.partner = self.chip * 2 + 1 - self.core

    def greet(self):
        barrier = pltpu.get_barrier_semaphore()
        for peer in (self.right, self.left, self.partner):
            pl.semaphore_signal(barrier, inc=1, device_id={"dp": peer}, device_id_type=MESH)
        pl.semaphore_wait(barrier, 3)


def _halves(rows):
    return pl.ds(0, rows // 2), pl.ds(rows // 2, rows // 2)


class Gather:
    def __init__(self, n, given, schedule, in_vmem=False):
        self.n, self.given, self.schedule = n, given, schedule
        self.inputs = [a for a, _ in given]
        shapes = [(n, *a.shape[1:]) for a, _ in given]
        self.out_shape = [] if in_vmem else [_like(s) for s in shapes]
        self.scratch = [pltpu.SemaphoreType.DMA((len(given), SLOTS))] * 2 + [pltpu.VMEM(s if in_vmem else s[1:], BF16) for s in shapes]

    def bind(self, ins, outs, scratch):
        self.send, self.recv = scratch[:2]
        self.src = [ref.at[layer] for ref, (_, layer) in zip(ins, self.given)]
        self.dst, self.own = (outs, scratch[2:]) if outs else (scratch[2:], None)
        self.place = _Place(self.n)
        return self

    def _copy(self, i, slot):
        p, src, dst = self.place, self.src[i], self.dst[i]
        first, second = _halves(src.shape[0])
        sends = {
            0: (src, dst.at[p.me], p.right),
            1: (src, dst.at[p.me], p.left),
            2: (src, dst.at[p.me], p.partner),
            3: (dst.at[p.left, first], dst.at[p.left, first], p.right),
            4: (dst.at[p.right, second], dst.at[p.right, second], p.left),
            5: (dst.at[p.left], dst.at[p.left], p.partner),
            6: (dst.at[p.right], dst.at[p.right], p.partner),
            7: (dst.at[p.across], dst.at[p.across], p.partner),
        }
        if slot == 8:
            return pltpu.make_async_copy(src, self.own[i] if self.own else dst.at[p.me], self.send.at[i, 8])
        if slot == 9:
            return pltpu.make_async_copy(self.own[i], dst.at[p.me], self.recv.at[i, 8])
        a, b, to = sends[slot]
        return pltpu.make_async_remote_copy(a, b, self.send.at[i, slot], self.recv.at[i, slot], device_id={"dp": to}, device_id_type=MESH)

    def start(self, i):
        for slot in (0, 1, 2, 8):
            self._copy(i, slot).start()

    def relay(self, i):
        for arrived, on in ((0, (3, 5)), (1, (4, 6))):
            self._copy(i, arrived).wait_recv()
            for slot in on:
                self._copy(i, slot).start()
        if self.own:
            self._copy(i, 8).wait()
            self._copy(i, 9).start()

    def cross(self, i):
        self._copy(i, 3).wait_recv()
        self._copy(i, 4).wait_recv()
        self._copy(i, 7).start()

    def finish(self, i):
        for slot in (2, 5, 6, 7):
            self._copy(i, slot).wait_recv()
        for slot in range(8):
            self._copy(i, slot).wait_send()
        self._copy(i, 9 if self.own else 8).wait()

    def at(self, point):
        _run(self, point)


class Scatter:
    def __init__(self, n, grads, schedule):
        self.n, self.schedule = n, schedule
        chips = n // 2
        blocks = [(g.shape[0] // n, g.shape[1]) for g in grads]
        self.count = len(grads)
        self.inputs = [g.reshape(chips, 2, *b) for g, b in zip(grads, blocks)]
        self.out_shape = [_like(b) for b in blocks]
        self.scratch = [pltpu.SemaphoreType.DMA((self.count, SLOTS))] * 2
        for r, c in blocks:
            self.scratch += [pltpu.VMEM((chips, r, c), BF16)] * 2 + [pltpu.VMEM((r, c), BF16)] * 2 + [pltpu.VMEM((r // 2, c), BF16)] * 2

    def bind(self, ins, outs, scratch):
        self.send, self.recv = scratch[:2]
        self.ins, self.outs = ins, outs
        self.bufs = [scratch[2 + 6 * i : 8 + 6 * i] for i in range(self.count)]
        self.place = _Place(self.n)
        return self

    def _copy(self, i, slot):
        p = self.place
        own, got, from_left, from_right, mid_left, mid_right = self.bufs[i]
        first, second = _halves(from_left.shape[0])
        if slot == 7:
            return pltpu.make_async_copy(from_left, self.outs[i], self.send.at[i, 7])
        if slot == 8:
            return pltpu.make_async_copy(self.ins[i].at[:, p.core], own, self.send.at[i, 8])
        a, b, to = {
            0: (self.ins[i].at[:, 1 - p.core], got, p.partner),
            1: (own.at[p.across_chip, first], mid_left, p.right),
            2: (own.at[p.across_chip, second], mid_right, p.left),
            3: (own.at[p.right_chip, second], from_left.at[second], p.right),
            4: (own.at[p.left_chip, first], from_right.at[first], p.left),
            5: (own.at[p.right_chip, first], from_left.at[first], p.right),
            6: (own.at[p.left_chip, second], from_right.at[second], p.left),
        }[slot]
        return pltpu.make_async_remote_copy(a, b, self.send.at[i, slot], self.recv.at[i, slot], device_id={"dp": to}, device_id_type=MESH)

    def start(self, i):
        self._copy(i, 0).start()
        self._copy(i, 8).start()

    def pair(self, i):
        own, got = self.bufs[i][:2]
        self._copy(i, 8).wait()
        self._copy(i, 0).wait_recv()

        def add(j, _):
            own[j] = (own[j].astype(F32) + got[j].astype(F32)).astype(BF16)

        lax.fori_loop(0, self.place.chips, add, None)
        self._copy(i, 1).start()
        self._copy(i, 2).start()

    def mid(self, i):
        p = self.place
        own, _, _, _, mid_left, mid_right = self.bufs[i]
        first, second = _halves(own.shape[1])
        for slot, chip, half, arrived in ((1, p.right_chip, first, mid_left), (2, p.left_chip, second, mid_right)):
            self._copy(i, slot).wait_recv()
            own[chip, half] = (own[chip, half].astype(F32) + arrived[...].astype(F32)).astype(BF16)
        for slot in (5, 6, 3, 4):
            self._copy(i, slot).start()

    def final(self, i):
        own, _, from_left, from_right, _, _ = self.bufs[i]
        for slot in (3, 4, 5, 6):
            self._copy(i, slot).wait_recv()
        total = own[self.place.chip].astype(F32) + from_left[...].astype(F32) + from_right[...].astype(F32)
        from_left[...] = total.astype(BF16)
        self._copy(i, 7).start()

    def finish(self, i):
        for slot in range(7):
            self._copy(i, slot).wait_send()
        self._copy(i, 7).wait()

    def at(self, point):
        _run(self, point)


def _run(plan, point):
    for name, items in plan.schedule.get(point, ()):
        _act(plan, name, items)


def _act(plan, name, items):
    if name == "greet":
        plan.place.greet()
    for i in items:
        getattr(plan, name)(i)


def _point(plan, t, steps, *rest):
    for step in range(steps):
        key = (step, *rest) if rest else step
        if key in plan.schedule:
            pl.when(t == step)(functools.partial(plan.at, key))


class _Idle:
    inputs, out_shape, scratch, schedule = [], [], [], {}

    def bind(self, *_):
        return self

    def at(self, point):
        pass


IDLE = _Idle()


def call(kernel, plan, number, *, grid, given, in_specs, out_specs, out_shape, scratch, cost):
    sizes = [len(given), len(plan.inputs), len(out_shape), len(plan.out_shape), len(scratch), len(plan.scratch)]
    ends = [sum(sizes[:i]) for i in range(7)]

    def body(*refs):
        a, b, c, d, e, f = (refs[ends[i] : ends[i + 1]] for i in range(6))
        kernel(plan.bind(b, d, f), *a, *c, *e)

    more = dict(collective_id=number, has_side_effects=True) if plan.inputs else {}
    got = pl.pallas_call(
        body,
        grid=grid,
        in_specs=in_specs + [ANY] * sizes[1],
        out_specs=out_specs + [ANY] * sizes[3],
        out_shape=out_shape + plan.out_shape,
        scratch_shapes=scratch + plan.scratch,
        compiler_params=_params(**more),
        cost_estimate=cost,
    )(*given, *plan.inputs)
    return got[: sizes[2]], got[sizes[2] :]


def adamw(w, m, v, g):
    m = 0.9 * m + 0.1 * g
    v = 0.95 * v + 0.05 * g * g
    step = m * lax.rsqrt(v + 1e-8) + 0.1 * w
    return (w - 0.02 * step).astype(BF16), m, v


class Both:
    def __init__(self, plans, schedule):
        self.plans, self.schedule = plans, schedule
        self.inputs, self.out_shape, self.scratch = (sum((getattr(p, x) for p in plans), []) for x in ("inputs", "out_shape", "scratch"))

    def bind(self, ins, outs, scratch):
        for p in self.plans:
            a, b, c = len(p.inputs), len(p.out_shape), len(p.scratch)
            p.bind(ins[:a], outs[:b], scratch[:c])
            ins, outs, scratch = ins[a:], outs[b:], scratch[c:]
        return self

    def at(self, point):
        for number, name, items in self.schedule.get(point, ()):
            _act(self.plans[number], name, items)


def _blocks(plan, block, causal_part, diagonal):
    iq, steps = pl.program_id(0), 4
    named = {i * (i + 1) // 2 + j: (i, j) for i in range(steps) for j in range(i + 1)}

    def ahead(inside, j=None):
        for number, (i, at) in named.items():
            if number in plan.schedule and (at < i) == inside:
                pl.when((iq == i) & (j == at) if inside else iq == i)(functools.partial(plan.at, number))

    def loop(j, _):
        ahead(True, j)
        causal_part(pl.multiple_of(j * block, block))

    lax.fori_loop(0, iq, loop, None)
    ahead(False)
    diagonal()


def _triangle(keys, queries):
    return lax.broadcasted_iota(jnp.int32, (keys, queries), 1) >= lax.broadcasted_iota(jnp.int32, (keys, queries), 0)


def _attend_kernel(plan, h_ref, cs_ref, *rest, scale, block, early):
    iq = pl.program_id(0)
    if "start" in plan.schedule:
        pl.when(iq == 0)(lambda: plan.at("start"))
    if early:
        wq_ref, wk_ref, wv_ref = (ref.reshape(-1, ref.shape[2]) for ref in plan.plans[0].dst)
    else:
        wq_ref, wk_ref, wv_ref, *rest = rest
    q_ref, k_out, v_out, o_ref, lse_ref, k_ref, v_ref, top_s, mix_s = rest
    here = pl.ds(pl.multiple_of(iq * block, block), block)
    wide = h_ref[...].astype(F32)
    a = (wide * _scale(wide)).astype(BF16)
    c, s = _turns(cs_ref[...])
    v = _dot(a, wv_ref[...], NN).astype(BF16)
    v_out[...] = v
    v_ref[here, :] = v
    q_ref[...] = _turn(_dot(a, wq_ref[...], NN).astype(BF16).astype(F32), c, s).astype(BF16)
    k = _turn(_dot(a, wk_ref[...], NN).astype(BF16).astype(F32), c, s).astype(BF16)
    k_out[...] = k
    k_ref[here, :] = k
    heads = q_ref.shape[1] // HEAD
    e = scale * LOG2E
    lanes = [slice(i * HEAD, (i + 1) * HEAD) for i in range(heads)]
    top_s[...] = jnp.full(top_s.shape, NEG, F32)
    mix_s[...] = jnp.zeros_like(mix_s)

    def part(key, keys, query, queries, masked):
        here, cols = pl.ds(key, keys), slice(query, query + queries)
        scores = [_dot(k_ref[here, x], q_ref[cols, x], NT) for x in lanes]
        ok = _triangle(keys, queries) if masked else None
        ones = jnp.ones((8, keys), BF16)
        weights, keeps = [], []
        for i, s in enumerate(scores):
            if masked:
                s = jnp.where(ok, s, HIDDEN)
            old = top_s[i : i + 1, cols]
            top = jnp.maximum(old, s.max(axis=0, keepdims=True))
            top_s[i : i + 1, cols] = top
            weights.append(jnp.exp2((s - top) * e).astype(BF16))
            keeps.append(jnp.exp2((old - top) * e))
        for i, (p, keep) in enumerate(zip(weights, keeps)):
            values = jnp.concatenate([v_ref[here, lanes[i]].T, ones], axis=0)
            mix_s[i, :, cols] = mix_s[i, :, cols] * keep + _dot(values, p, NN)

    half = block // 2
    base = pl.multiple_of(iq * block, block)

    def diagonal():
        part(base, half, 0, block, True)
        part(pl.multiple_of(base + half, half), half, half, half, True)

    _blocks(plan, block, lambda key: part(key, block, 0, block, False), diagonal)
    for i, x in enumerate(lanes):
        total = mix_s[i, HEAD : HEAD + 1, :]
        o_ref[:, x] = (mix_s[i, :HEAD, :] * (1 / total)).T.astype(BF16)
        lse_ref[i : i + 1, :] = top_s[i : i + 1, :] * scale + jnp.log(total)
    if "end" in plan.schedule:
        pl.when(iq == pl.num_programs(0) - 1)(lambda: plan.at("end"))


def attend(h, cs, ws, width, plan=IDLE, number=0):
    tokens, d = h.shape
    heads, block = width // HEAD, tokens // 4
    early = ws is None
    return call(
        functools.partial(_attend_kernel, scale=HEAD**-0.5, block=block, early=early), plan, number,
        grid=(tokens // block,),
        given=[h, cs] + list(ws or ()),
        in_specs=[_rows(block, d), _rows(block, HEAD)] + [_whole((d, width))] * (0 if early else 3),
        out_specs=[_rows(block, width)] * 4 + [pl.BlockSpec((heads, block), lambda t: (0, t))],
        out_shape=[_like((tokens, width))] * 4 + [_like((heads, tokens), F32)],
        scratch=[pltpu.VMEM((tokens, width), BF16)] * 2 + [pltpu.VMEM((heads, block), F32), pltpu.VMEM((heads, HEAD + 8, block), F32)],
        cost=_cost(4 * heads * tokens * tokens * HEAD + 6 * tokens * d * width, h, h, h, h, h, exps=heads * tokens * tokens),
    )


def _ffn_kernel(plan, o_ref, h_ref, wo_ref, wg_ref, wu_ref, wd_ref, h1_ref, h2_ref, g_ref, u_ref, *, chunk):
    t = pl.program_id(0)
    _point(plan, t, 4, 0)
    h1 = (h_ref[...].astype(F32) + _dot(o_ref[...], wo_ref[...], NN).astype(BF16).astype(F32)).astype(BF16)
    h1_ref[...] = h1
    wide = h1.astype(F32)
    b = (wide * _scale(wide)).astype(BF16)
    total = None
    for at in range(0, wg_ref.shape[1], chunk):
        here = slice(at, at + chunk)
        if at:
            _point(plan, t, 4, at // chunk)
        gate, up = _dot(b, wg_ref[:, here], NN), _dot(b, wu_ref[:, here], NN)
        g_ref[:, here] = gate
        u_ref[:, here] = up
        act = (gate * jax.nn.sigmoid(gate) * up).astype(BF16)
        term = _dot(act, wd_ref[here, :], NN)
        total = term if total is None else total + term
    h2_ref[...] = (wide + total.astype(BF16).astype(F32)).astype(BF16)
    if "end" in plan.schedule:
        pl.when(t == pl.num_programs(0) - 1)(lambda: plan.at("end"))


def ffn(o, h, wo, wg, wu, wd, plan=IDLE, number=0, chunk=512, parts=4):
    tokens, d = h.shape
    width, hidden, tile = o.shape[1], wg.shape[1], tokens // parts
    return call(
        functools.partial(_ffn_kernel, chunk=chunk), plan, number,
        grid=(tokens // tile,),
        given=[o, h, wo, wg, wu, wd],
        in_specs=[_rows(tile, width), _rows(tile, d)] + [_whole(w.shape) for w in (wo, wg, wu, wd)],
        out_specs=[_rows(tile, d)] * 2 + [_rows(tile, hidden)] * 2,
        out_shape=[_like((tokens, d))] * 2 + [_like((tokens, hidden), F32)] * 2,
        scratch=[],
        cost=_cost(2 * tokens * d * (width + 3 * hidden), o, h, h, h, wo, wg, wu, wd),
    )


STRIP = 64


def _by_rows(ref, act):
    lax.fori_loop(0, ref.shape[0] // STRIP, lambda i, _: act(pl.ds(pl.multiple_of(i * STRIP, STRIP), STRIP)), None)


def _ffn_bwd_kernel(plan, dh2_ref, o_ref, *rest, chunk, last):
    if last:
        h_ref, *rest = rest
    else:
        h1_ref, g_ref, u_ref, *rest = rest
    wo_ref, wg_ref, wu_ref, wd_ref, dh1_ref, do_ref, dwo_ref, dwg_ref, dwu_ref, dwd_ref, awo, awg, awu, awd, db_s = rest
    t = pl.program_id(0)
    _point(plan, t, 4, 0)

    @pl.when(t == 0)
    def _():
        for acc in (awo, awg, awu, awd):
            _by_rows(acc, lambda rows, acc=acc: acc.__setitem__(rows, jnp.zeros((STRIP, acc.shape[1]), F32)))

    dh2, o = dh2_ref[...], o_ref[...]
    if last:
        wide = (h_ref[...].astype(F32) + _dot(o, wo_ref[...], NN).astype(BF16).astype(F32)).astype(BF16).astype(F32)
    else:
        wide = h1_ref[...].astype(F32)
    scale = _scale(wide)
    b = (wide * scale).astype(BF16)
    b_t = b.T
    db_s[...] = jnp.zeros_like(db_s)

    def hidden(at, _):
        here = pl.ds(pl.multiple_of(at * chunk, chunk), chunk)
        d_act = _dot(dh2, wd_ref[here, :], NT).astype(BF16).astype(F32)
        if last:
            gate, up = _dot(b, wg_ref[:, here], NN), _dot(b, wu_ref[:, here], NN)
        else:
            gate, up = g_ref[:, here], u_ref[:, here]
        sig = jax.nn.sigmoid(gate)
        silu = gate * sig
        act = (silu * up).astype(BF16)
        d_up = (d_act * silu).astype(BF16)
        d_gate = (d_act * up * (sig + silu * (1 - sig))).astype(BF16)
        db_s[...] += _dot(d_gate, wg_ref[:, here], NT) + _dot(d_up, wu_ref[:, here], NT)
        awd[here, :] += _dot(act.T, dh2, NN)
        awg[:, here] += _dot(b_t, d_gate, NN)
        awu[:, here] += _dot(b_t, d_up, NN)

    lax.fori_loop(0, wg_ref.shape[1] // chunk, hidden, None)
    db = db_s[...].astype(BF16).astype(F32)
    dh1 = (dh2.astype(F32) + _norm_bwd(wide, scale, db).astype(BF16).astype(F32)).astype(BF16)
    dh1_ref[...] = dh1
    do_ref[...] = _dot(dh1, wo_ref[...], NT).astype(BF16)
    awo[...] += _dot(o.T, dh1, NN)

    @pl.when(t == pl.num_programs(0) - 1)
    def _():
        for out, acc in ((dwo_ref, awo), (dwg_ref, awg), (dwu_ref, awu), (dwd_ref, awd)):
            _by_rows(acc, lambda rows, out=out, acc=acc: out.__setitem__(rows, acc[rows].astype(BF16)))
        plan.at("end")


def ffn_bwd(dh2, o, acts, wo, wg, wu, wd, plan=IDLE, number=0, chunk=512, parts=4):
    tokens, d = dh2.shape
    width, hidden, tile = o.shape[1], wg.shape[1], tokens // parts
    ws = (wo, wg, wu, wd)
    last = len(acts) == 1
    return call(
        functools.partial(_ffn_bwd_kernel, chunk=chunk, last=last), plan, number,
        grid=(tokens // tile,),
        given=[dh2, o, *acts, *ws],
        in_specs=[_rows(tile, d), _rows(tile, width)] + [_rows(tile, a.shape[1]) for a in acts] + [_whole(w.shape) for w in ws],
        out_specs=[_rows(tile, d), _rows(tile, width)] + [_whole(w.shape) for w in ws],
        out_shape=[_like((tokens, d)), _like((tokens, width))] + [_like(w.shape) for w in ws],
        scratch=[pltpu.VMEM(w.shape, F32) for w in ws] + [pltpu.VMEM((tile, d), F32)],
        cost=_cost(4 * tokens * d * (width + 3 * hidden), *acts, dh2, o, *ws, *ws),
    )


def _attend_bwd_kernel(plan, q_ref, k_ref, v_ref, do_ref, o_ref, lse_ref, dq_ref, dk_ref, dv_ref, dq_s, dk_s, dv_s, *, scale, block):
    iq = pl.program_id(0)
    if "start" in plan.schedule:
        pl.when(iq == 0)(lambda: plan.at("start"))
    heads = q_ref.shape[1] // HEAD
    e = scale * LOG2E
    lanes = [slice(i * HEAD, (i + 1) * HEAD) for i in range(heads)]

    @pl.when(iq == 0)
    def _():
        dk_s[...] = jnp.zeros_like(dk_s)
        dv_s[...] = jnp.zeros_like(dv_s)

    dq_s[...] = jnp.zeros_like(dq_s)
    lses = [lse_ref[i : i + 1, :] * LOG2E for i in range(heads)]
    deltas = [(do_ref[:, x].astype(F32) * o_ref[:, x].astype(F32)).T.sum(axis=0, keepdims=True) for x in lanes]

    def part(key, keys, query, queries, masked):
        here, cols = pl.ds(key, keys), slice(query, query + queries)
        scores = [_dot(k_ref[here, x], q_ref[cols, x], NT) for x in lanes]
        dps = [_dot(v_ref[here, x], do_ref[cols, x], NT) for x in lanes]
        ok = _triangle(keys, queries) if masked else None
        for i, x in enumerate(lanes):
            p = jnp.exp2(scores[i] * e - lses[i][:, cols])
            if masked:
                p = jnp.where(ok, p, 0.0)
            ds = (p * (dps[i] - deltas[i][:, cols])).astype(BF16)
            dv_s[here, x] += _dot(p.astype(BF16), do_ref[cols, x], NN)
            dk_s[here, x] += _dot(ds, q_ref[cols, x], NN)
            dq_s[i, :, cols] += _dot(k_ref[here, x].T, ds, NN)

    half = block // 2
    base = pl.multiple_of(iq * block, block)

    def diagonal():
        part(base, half, 0, block, True)
        part(pl.multiple_of(base + half, half), half, half, half, True)

    _blocks(plan, block, lambda key: part(key, block, 0, block, False), diagonal)
    for i, x in enumerate(lanes):
        dq_ref[:, x] = (dq_s[i] * scale).T.astype(BF16)

    @pl.when(iq == pl.num_programs(0) - 1)
    def _():
        dk_ref[...] = (dk_s[...] * scale).astype(BF16)
        dv_ref[...] = dv_s[...].astype(BF16)
        plan.at("end")


def attend_bwd(q, k, v, do, o, lse, plan=IDLE, number=0):
    tokens, width = q.shape
    heads, block = width // HEAD, tokens // 4
    return call(
        functools.partial(_attend_bwd_kernel, scale=HEAD**-0.5, block=block), plan, number,
        grid=(tokens // block,),
        given=[q, k, v, do, o, lse],
        in_specs=[_rows(block, width), _whole(k.shape), _whole(v.shape), _rows(block, width), _rows(block, width),
                  pl.BlockSpec((heads, block), lambda t: (0, t))],
        out_specs=[_rows(block, width), _whole(k.shape), _whole(v.shape)],
        out_shape=[_like((tokens, width))] * 3,
        scratch=[pltpu.VMEM((heads, HEAD, block), F32), pltpu.VMEM(k.shape, F32), pltpu.VMEM(v.shape, F32)],
        cost=_cost(10 * heads * tokens * tokens * HEAD, q, k, v, do, o, q, k, v, exps=heads * tokens * tokens),
    )


def _qkv_bwd_kernel(plan, h_ref, cs_ref, dq_ref, dk_ref, dv_ref, *rest, inner, updates):
    layers = rest[0].shape[0] if updates else 0
    per = 3 + layers
    states, rest = rest[: per * updates], rest[per * updates :]
    results, rest = rest[3 : 3 + 3 * updates], rest[:3] + rest[3 + 3 * updates :]
    for i in range(updates):
        w_ref, m_ref, v_ref, *gs = states[per * i : per * i + per]
        for at, g_ref in enumerate(gs):
            new = adamw(w_ref[at].astype(F32), m_ref[at], v_ref[at], g_ref[...].astype(F32))
            for out, one in zip(results[3 * i : 3 * i + 3], new):
                out[at] = one
    if inner:
        dh1_ref, wq_ref, wk_ref, wv_ref, dh_ref, dwq_ref, dwk_ref, dwv_ref, *accs = rest
    else:
        dwq_ref, dwk_ref, dwv_ref, *accs = rest
    t = pl.program_id(0)
    _point(plan, t, 4)

    @pl.when(t == 0)
    def _():
        for acc in accs:
            acc[...] = jnp.zeros_like(acc)

    wide = h_ref[...].astype(F32)
    scale = _scale(wide)
    a = (wide * scale).astype(BF16)
    c, s = _turns(cs_ref[...])
    grads = [_turn(ref[...].astype(F32), c, -s).astype(BF16) for ref in (dq_ref, dk_ref)] + [dv_ref[...]]
    a_t = a.T
    for acc, g in zip(accs, grads):
        acc[...] += _dot(a_t, g, NN)
    if inner:
        da = sum(_dot(g, w[...], NT) for g, w in zip(grads, (wq_ref, wk_ref, wv_ref)))
        da = da.astype(BF16).astype(F32)
        dh_ref[...] = (dh1_ref[...].astype(F32) + _norm_bwd(wide, scale, da).astype(BF16).astype(F32)).astype(BF16)

    @pl.when(t == pl.num_programs(0) - 1)
    def _():
        for out, acc in zip((dwq_ref, dwk_ref, dwv_ref), accs):
            out[...] = acc[...].astype(BF16)
        plan.at("end")


def qkv_bwd(h, cs, dq, dk, dv, dh1=None, ws=None, updates=(), plan=IDLE, number=0, parts=4):
    tokens, d = h.shape
    width, tile = dq.shape[1], tokens // parts
    inner = dh1 is not None
    given = [h, cs, dq, dk, dv] + ([dh1, *ws] if inner else [])
    specs = [_rows(tile, d), _rows(tile, HEAD)] + [_rows(tile, width)] * 3 + ([_rows(tile, d)] + [_whole((d, width))] * 3 if inner else [])
    outs, shapes = [], []
    for w, m, v, *gs in updates:
        layers, rows, columns = w.shape
        cut = pl.BlockSpec((layers, rows // parts, columns), lambda t: (0, t, 0))
        given += [w, m, v, *gs]
        specs += [cut] * 3 + [_rows(rows // parts, columns)] * layers
        outs += [cut] * 3
        shapes += [_like(w.shape), _like(w.shape, F32), _like(w.shape, F32)]
    return call(
        functools.partial(_qkv_bwd_kernel, inner=inner, updates=len(updates)), plan, number,
        grid=(tokens // tile,),
        given=given,
        in_specs=specs,
        out_specs=([_rows(tile, d)] if inner else []) + [_whole((d, width))] * 3 + outs,
        out_shape=([_like((tokens, d))] if inner else []) + [_like((d, width))] * 3 + shapes,
        scratch=[pltpu.VMEM((d, width), F32)] * 3,
        cost=_cost((12 if inner else 6) * tokens * d * width, *given),
    )


def _tail_kernel(plan):
    for point in range(4):
        plan.at(point)


def solution(mesh):
    n = mesh.shape["dp"]

    def flat(w):
        return w.reshape(-1, w.shape[2])

    def step(x, dy, *arrays):
        weights, m, v = (arrays[i : i + 7] for i in (0, 7, 14))
        wq, wk, wv, wo, wg, wu, wd = weights
        layers, width = wq.shape[0], wq.shape[2]
        h = x[0]
        cs = jnp.asarray(_table(h.shape[0]))
        layer = [dict(zip(NAMES, (None,) * 7)) for _ in range(layers)]

        def gathering(names, number, schedule, **more):
            return Gather(n, [(weights[NAMES.index(name)], number) for name in names], schedule, **more)

        def arrived(number, names, got):
            layer[number].update({name: flat(one) for name, one in zip(names, got)})

        def of(number, names):
            return [layer[number][name] for name in names]

        greet = ("greet", ())
        FFN, QKV = ("wo", "wg", "wu", "wd"), ("wq", "wk", "wv")
        kept = []
        for i in range(layers):
            if i == 0:
                names, ws = FFN, None
                plan = Both([gathering(QKV, 0, {}, in_vmem=True), gathering(names, 0, {})],
                            {"start": [(0, *greet), (0, "start", range(3)), (0, "relay", range(3)), (1, "start", (0, 1)), (0, "cross", range(3)),
                                       (1, "start", (2, 3)), (0, "finish", range(3))],
                             2: [(1, "relay", (0, 1))], 5: [(1, "relay", (2, 3))], 8: [(1, "cross", (0, 1))],
                             "end": [(1, "cross", (2, 3)), (1, "finish", range(4))]})
            else:
                names, ws = ("wg", "wu"), of(i, QKV)
                plan = gathering(names, i, {"start": [greet, ("start", (0, 1))], 5: [("relay", (0, 1))], 9: [("cross", (0,))],
                                            "end": [("cross", (1,)), ("finish", (0, 1))]})
            (q, k, v_, o, lse), got = attend(h, cs, ws, width, plan, 2 + 2 * i)
            arrived(i, names, got)
            if i + 1 < layers:
                names = (*QKV, "wo", "wd")
                plan = gathering(names, i + 1, {(0, 0): [greet, ("start", range(5))], (2, 2): [("relay", range(5))], (3, 3): [("cross", range(4))],
                                                "end": [("cross", (4,)), ("finish", range(5))]})
                (h1, h2, g, u), got = ffn(o, h, *of(i, FFN), plan, 3 + 2 * i)
                arrived(i + 1, names, got)
                kept.append((h, q, k, v_, o, lse, (h1, g, u)))
                h = h2
            else:
                kept.append((h, q, k, v_, o, lse, (h,)))
        dh, mine = dy[0], {}

        def scattering(pairs, schedule):
            return Scatter(n, [one for _, one in pairs], schedule)

        def done(pairs, got):
            mine.update({key: one for (key, _), one in zip(pairs, got)})

        waiting = []
        for i in reversed(range(layers)):
            h, q, k, v_, o, lse, acts = kept[i]
            every = range(len(waiting))
            plan = scattering(waiting, {(0, 0): [greet, ("start", every)], (1, 0): [("pair", every)], (2, 0): [("mid", every)],
                                        "end": [("final", every), ("finish", every)]}) if waiting else IDLE
            (dh1, do, dwo, dwg, dwu, dwd), got = ffn_bwd(dh, o, acts, *of(i, FFN), plan, 20 + 3 * i)
            done(waiting, got)
            rest = [(("wo", i), dwo)]
            now = [(("wg", i), dwg), (("wu", i), dwu), (("wd", i), dwd)]
            if i:
                rest, now = [now[2]] + rest, now[:2]
            more = range(1, len(now))
            points = {"start": [greet, ("start", (0,))], 1: [("pair", (0,)), ("start", more)], 2: [("pair", more)], 3: [("mid", (0,))],
                      5: [("mid", more)], 7: [("final", (0,))], "end": [("final", more), ("finish", range(len(now)))]}
            (dq, dk, dv), got = attend_bwd(q, k, v_, do, o, lse, scattering(now, points), 21 + 3 * i)
            done(now, got)
            if i:
                (dh, *grads), _ = qkv_bwd(h, cs, dq, dk, dv, dh1, of(i, QKV))
            else:
                updates = [(weights[k], m[k], v[k], *(mine[NAMES[k], j] for j in range(layers))) for k in (4, 5, 6)]
                (*grads, a, b, c, d, e, f, x_, y_, z_), _ = qkv_bwd(h, cs, dq, dk, dv, updates=updates)
                ffn_new = [(a, b, c), (d, e, f), (x_, y_, z_)]
            waiting = rest + [((name, i), one) for name, one in zip(QKV, grads)]
        every = range(len(waiting))
        plan = scattering(waiting, {0: [greet, ("start", every)], 1: [("pair", every)], 2: [("mid", every)],
                                    3: [("final", every), ("finish", every)]})
        _, got = call(_tail_kernel, plan, 18, grid=(), given=[], in_specs=[], out_specs=[], out_shape=[], scratch=[], cost=None)
        done(waiting, got)
        gradients = [jnp.stack([mine[name, i] for i in range(layers)]).astype(F32) for name in NAMES[:4]]
        new = [adamw(w.astype(F32), m, v, g) for w, m, v, g in zip(weights[:4], m[:4], v[:4], gradients, strict=True)] + ffn_new
        return tuple(one[which] for which in range(3) for one in new)

    states, cut = P(("rep", "dp"), None, None), P(None, "dp", None)
    return jax.shard_map(
        step,
        mesh=mesh,
        in_specs=(states, states) + (cut,) * 21,
        out_specs=(P("rep", "dp", None),) * 21,
        check_vma=False,
    )
```
